512 devices in a mesh: det: 128 (over y, z, core), row: 4 (over x).
Axes of the slice: x: 4, y: 8, z: 8, core: 2. Of those that a mesh axis runs over, the one named last changes fastest.
Arguments:
- science: float32 [128, 128, 768], P('det', 'row'), may hold values from -6 to 6
- template: float32 [128, 6, 128, 128], P('det', None, 'row'), may hold values from -6 to 6
- tile_source: int32 [128, 6], replicated, may hold values from 0 to 767, as said below
- offsets: int32 [2, 128, 6], P(None, 'det'), may hold values from 0 to 3
- shift_weights: float32 [2, 128, 6], P(None, 'det'), may hold values from 0 to 1
- valid_rows: int32 [128, 6], P('det'), may hold values from 32 to 128
- basis_kernels: float32 [27, 31, 31], replicated, may hold values from -0.1875 to 0.1875
- coefficients: float32 [128, 27], P('det'), may hold values from -1.25 to 1.25
- background: float32 [128], P('det'), may hold values from -4 to 4
Outputs:
- difference_tiles: float32 [128, 6, 128, 128], P('det', None, 'row')
The draws below stay inside these ranges and needn't reach their ends.
Inputs may be any that keep to these rules, and one draw needn't show every extreme that they name: `tile_source`: entry [d, c] names slot s of sky patch p as p * 6 + s. Row d names the patches (d + j) mod 128 for j = 0 .. 3, in that order along the columns, each in one run of consecutive columns that names consecutive slots, 1 to 3 tiles long; one run of each row is exactly 3 long.
All inputs are finite; a program needn't handle non-finite values.
Results may differ from the reference program's by a relative error of at most 0.000062.
Values sent between devices are 32-bit elements; how exact they have to be, the bound alone decides.
A program may use at most 64 MiB of HBM per device.

```python
import jax
import jax.numpy as jnp
from jax import lax

TILE = 128
TC = 6
KW = 31
NB = 27
MAXOFF = 4
SPAN = 4
DETS = 128
W = 768
PT_DEV = 6
CAP = 3
HALF = 15


def route_table(key):
    first_key, second_key, third_key, fourth_key = jax.random.split(jax.random.fold_in(key, 7), 4)
    lower_cut = jax.random.randint(first_key, (DETS,), 1, CAP - 1).astype(jnp.int32)
    upper_cut = jax.random.randint(second_key, (DETS,), lower_cut + 1, CAP).astype(jnp.int32)
    remaining = jnp.stack([lower_cut, upper_cut - lower_cut, CAP - upper_cut], axis=1).astype(jnp.int32)
    longest = jax.random.randint(third_key, (DETS, 1), 0, SPAN).astype(jnp.int32)
    run_ids = jnp.arange(SPAN, dtype=jnp.int32)[None, :]
    rest_index = jnp.clip(run_ids - (run_ids > longest).astype(jnp.int32), 0, SPAN - 2)
    runs = jnp.where(run_ids == longest, jnp.int32(CAP), jnp.take_along_axis(remaining, rest_index, axis=1)).astype(jnp.int32)
    ends = jnp.cumsum(runs, axis=1).astype(jnp.int32)
    starts = (ends - runs).astype(jnp.int32)
    column_ids = jnp.arange(TC, dtype=jnp.int32)
    run_of = jnp.sum((column_ids[None, :, None] >= ends[:, None, :SPAN - 1]).astype(jnp.int32), axis=2).astype(jnp.int32)
    ranks = column_ids[None, :] - jnp.take_along_axis(starts, run_of, axis=1)
    slot_start = jax.random.randint(fourth_key, (DETS, SPAN), 0, PT_DEV - runs + 1).astype(jnp.int32)
    slots = jnp.take_along_axis(slot_start, run_of, axis=1) + ranks
    owners = (jnp.arange(DETS, dtype=jnp.int32)[:, None] + run_of) % DETS
    return (owners * PT_DEV + slots).astype(jnp.int32)


def draw_tile_source(key, part):
    return route_table(key)


def set_ends(values, stream_key, low, top_value):
    index_at = [jax.random.randint(jax.random.fold_in(stream_key, axis), (), 0, length) for axis, length in enumerate(values.shape)]
    main_axis = values.shape.index(max(values.shape))
    next_to = index_at[:main_axis] + [(index_at[main_axis] + 1) % values.shape[main_axis]] + index_at[main_axis + 1:]
    return values.at[tuple(index_at)].set(low).at[tuple(next_to)].set(top_value)


def shard_levels(stream_key, shape, cuts, least, largest):
    def one(axis_at, shards_of):
        draws = jax.random.uniform(jax.random.fold_in(jax.random.fold_in(stream_key, 6), axis_at), (shards_of,), jnp.float32, least / len(cuts), largest / len(cuts))
        return jnp.repeat(jnp.exp(draws), shape[axis_at] // shards_of).reshape((-1,) + (1,) * (len(shape) - axis_at - 1))

    level = one(*cuts[0])
    for cut in cuts[1:]:
        level = level * one(*cut)
    return level


def scatter_about(rng, dims, width, bound, shards=(), kind=jnp.bfloat16):
    factor_of = shard_levels(rng, dims, shards, -0.22, 0.18) if shards else 1.0
    values = jax.random.normal(rng, dims, jnp.float32) * width * factor_of
    return jnp.minimum(jnp.maximum(values, -bound), bound).astype(kind)


def setup_inputs(seed: int = 0) -> dict:
    keys = jax.random.split(jax.random.key(seed), 10)
    science = scatter_about(keys[0], (DETS, TILE, W), 1.0, 6.0, ((0, 128), (1, 4)), jnp.float32)
    template = scatter_about(keys[1], (DETS, PT_DEV, TILE, TILE), 1.0, 6.0, ((0, 128), (2, 4)), jnp.float32)
    tile_source = draw_tile_source(jax.random.fold_in(keys[9], 71), 0)
    offsets = set_ends(jax.random.randint(keys[3], (2, DETS, TC), 0, MAXOFF), jax.random.fold_in(keys[3], 1), 0, MAXOFF - 1).astype(jnp.int32)
    shift_weights = jnp.clip(1.0 * jax.random.uniform(keys[4], (2, DETS, TC), jnp.float32) ** shard_levels(keys[4], (2, DETS, TC), ((1, 128),), -0.2, 0.2), 0.0, 1.0)
    valid_rows = set_ends(jax.random.randint(keys[5], (DETS, TC), TILE // 4, TILE + 1), jax.random.fold_in(keys[5], 1), TILE // 4, TILE).astype(jnp.int32)
    basis_kernels = scatter_about(keys[6], (NB, KW, KW), (KW * KW) ** -0.5, 0.1875, (), jnp.float32)
    coefficients = scatter_about(keys[7], (DETS, NB), NB ** -0.5, 1.25, ((0, 128),), jnp.float32)
    background = scatter_about(keys[8], (DETS,), 1.0, 4.0, ((0, 128),), jnp.float32)
    return dict(science=science, template=template, tile_source=tile_source, offsets=offsets, shift_weights=shift_weights, valid_rows=valid_rows, basis_kernels=basis_kernels, coefficients=coefficients, background=background)


def convolve(pair):
    image, kernel = pair
    result = lax.conv_general_dilated(image[None, None], kernel[None, None], (1, 1), ((HALF, HALF), (HALF, HALF)), precision=lax.Precision.HIGHEST)
    return result[0, 0]


def reference(science, template, tile_source, offsets, shift_weights, valid_rows, basis_kernels, coefficients, background):
    flat_tiles = template.reshape(DETS * PT_DEV, TILE, TILE)
    sources = tile_source.reshape(-1).astype(jnp.int32)
    gathered = flat_tiles[sources]
    row_shift = offsets[0].reshape(-1).astype(jnp.int32)
    column_shift = offsets[1].reshape(-1).astype(jnp.int32)
    row_weight = shift_weights[0].reshape(-1)
    column_weight = shift_weights[1].reshape(-1)
    column_ids = jnp.arange(TILE, dtype=jnp.int32)
    first_cols = jnp.minimum(column_ids[None, :] + column_shift[:, None], TILE - 1)
    second_cols = jnp.minimum(column_ids[None, :] + column_shift[:, None] + 1, TILE - 1)
    left_part = jnp.take_along_axis(gathered, first_cols[:, None, :], axis=2)
    right_part = jnp.take_along_axis(gathered, second_cols[:, None, :], axis=2)
    across = (1.0 - column_weight)[:, None, None] * left_part + column_weight[:, None, None] * right_part
    padded = jnp.pad(across, ((0, 0), (0, MAXOFF + 1), (0, 0)))
    first_rows = column_ids[None, :] + row_shift[:, None]
    upper_part = jnp.take_along_axis(padded, first_rows[:, :, None], axis=1)
    lower_part = jnp.take_along_axis(padded, first_rows[:, :, None] + 1, axis=1)
    warped = (1.0 - row_weight)[:, None, None] * upper_part + row_weight[:, None, None] * lower_part
    warped = warped.reshape(DETS, TC, TILE, TILE).transpose(0, 2, 1, 3).reshape(DETS, TILE, W)
    kernels = jnp.einsum('dk,kab->dab', coefficients, basis_kernels, precision=lax.Precision.HIGHEST)
    modelled = lax.map(convolve, (warped, kernels))
    residual_image = science - modelled - background[:, None, None]
    limits = jnp.repeat(valid_rows.astype(jnp.int32), TILE, axis=1)
    inside = column_ids[None, :, None] < limits[:, None, :]
    residual_image = jnp.where(inside, residual_image, jnp.float32(0.0))
    pieces = residual_image.reshape(DETS, TILE, TC, TILE).transpose(0, 2, 1, 3).reshape(DETS * TC, TILE, TILE)
    summed = jax.ops.segment_sum(pieces, sources, num_segments=DETS * PT_DEV)
    tallies = jax.ops.segment_sum(jnp.ones(sources.shape, jnp.float32), sources, num_segments=DETS * PT_DEV)
    result = summed / jnp.maximum(tallies, 1.0)[:, None, None]
    return result.reshape(DETS, PT_DEV, TILE, TILE)
```

```python
import functools

import jax
import jax.numpy as jnp
from jax import lax
from jax.experimental import pallas as pl
from jax.experimental.pallas import tpu as pltpu
from jax.sharding import PartitionSpec as P

MESH = pl.DeviceIdType.MESH
SPAN = 4
CAP = 3
TILES = 6
TILE = 128
BAND = 32
ABOVE = 16
BELOW = 24
DEEP = ABOVE + BAND + BELOW
KW = 31
HALF = 15
NB = 27
MAXOFF = 4
ZERO_TILE = 12


def split(x):
    high = x.astype(jnp.bfloat16).astype(jnp.float32)
    return high, x - high


def kernel(
    det_count,
    row_count,
    science,
    template,
    sources,
    offsets,
    weights,
    valid,
    basis,
    coefs,
    background,
    out,
    own,
    tiles,
    edges,
    images,
    seen,
    bands,
    taps,
    taps_back,
    floats,
    ints,
    float_s,
    int_s,
    local_sem,
    send_sem,
    recv_sem,
):
    p = lax.axis_index("det")
    r = lax.axis_index("row")

    def det(j):
        return lax.rem(p + (j + det_count), det_count)

    def row(j):
        return lax.rem(r + (j + row_count), row_count)

    peers = [(det(j), r) for j in (1, -1, 2, -2, 3, -3)]
    peers += [(p, row(1)), (p, row(-1))]
    peers += [(det(j), row(i)) for j in (1, -1) for i in (1, -1)]
    barrier = pltpu.get_barrier_semaphore()
    for peer in peers:
        pl.semaphore_signal(barrier, inc=1, device_id=peer, device_id_type=MESH)

    load_own = pltpu.make_async_copy(template.at[0], own, local_sem.at[0])
    load_tiles = pltpu.make_async_copy(
        template.at[0], tiles.at[pl.ds(0, TILES), pl.ds(ABOVE, BAND), :], local_sem.at[1]
    )
    load_seen = pltpu.make_async_copy(
        science.at[0, :, pl.ds(0, CAP * TILE)], seen.at[0], local_sem.at[2]
    )
    load_own.start()
    load_tiles.start()
    load_seen.start()

    runs = []
    for q in range(SPAN):
        d = det(-q)
        start = jnp.int32(0)
        length = jnp.int32(0)
        for c in range(TILES):
            reach = lax.rem(sources[c, d] // TILES - d + det_count, det_count)
            start = start + jnp.where(reach < q, 1, 0)
            length = length + jnp.where(reach == q, 1, 0)
        start = jnp.clip(start, 0, TILES - 1)
        first = jnp.clip(sources[start, d] - p * TILES, 0, TILES - 1)
        runs.append((start, length, first))

    lane = lax.broadcasted_iota(jnp.int32, (1, TILE), 1)
    packed = jnp.zeros((1, TILE), jnp.float32)
    whole = jnp.zeros((1, TILE), jnp.int32)
    for k in range(NB):
        packed = jnp.where(lane == k, coefs[0, k], packed)
    packed = jnp.where(lane == NB, background[0], packed)
    for c in range(TILES):
        packed = jnp.where(lane == 28 + c, weights[0, 0, c], packed)
        packed = jnp.where(lane == 34 + c, weights[1, 0, c], packed)
        whole = jnp.where(lane == c, offsets[0, 0, c], whole)
        whole = jnp.where(lane == 6 + c, offsets[1, 0, c], whole)
        whole = jnp.where(lane == 12 + c, valid[0, c], whole)
    floats[0] = packed
    ints[0] = whole

    tiles[ZERO_TILE] = jnp.zeros((DEEP, TILE), jnp.float32)
    load_own.wait()
    for j in range(CAP):
        start, length, first = runs[j]
        edges[0, j] = own[jnp.clip(first + length - 1, 0, TILES - 1)]
        start, length, first = runs[j + 1]
        edges[1, j] = own[first]

    sub = lax.broadcasted_iota(jnp.int32, (8, TILE), 0)
    across = lax.broadcasted_iota(jnp.int32, (8, TILE), 1)
    rows128 = lax.broadcasted_iota(jnp.int32, (TILE, TILE), 0)
    cols128 = lax.broadcasted_iota(jnp.int32, (TILE, TILE), 1)
    mirror = jnp.where(lax.rem(rows128 + cols128, TILE) == 0, 1.0, 0.0).astype(jnp.float32)
    taps[...] = jnp.zeros((BAND, TILE), jnp.float32)

    def build(q, coefficient):
        total = coefficient(0) * basis[0]
        for k in range(1, NB):
            total = total + coefficient(k) * basis[k]
        taps[pl.ds(0, KW), pl.ds(0, KW)] = total
        high, low = split(taps[...])
        both = jnp.dot(
            jnp.concatenate([high, low], axis=0), mirror, preferred_element_type=jnp.float32
        )
        taps_back[...] = both[:BAND] + both[BAND:]
        for a in range(KW):
            line = jnp.broadcast_to(taps_back[pl.ds(a, 1), :], (8, TILE))
            block = pltpu.roll(line, 0, 1, stride=1, stride_axis=0)
            for jb in range(TILE // 8):
                turned = block if jb == 0 else pltpu.roll(block, 8 * jb, 1)
                high, low = split(turned)
                if jb < 4:
                    lead = across <= sub + 8 * jb
                    lead_high, lead_low = jnp.where(lead, high, 0.0), jnp.where(lead, low, 0.0)
                    bands[q, a, pl.ds(TILE + 8 * jb, 8), pl.ds(0, TILE)] = high - lead_high
                    bands[q, a, pl.ds(TILE + 8 * jb, 8), pl.ds(TILE, TILE)] = low - lead_low
                    high, low = lead_high, lead_low
                bands[q, a, pl.ds(8 * jb, 8), pl.ds(0, TILE)] = high
                bands[q, a, pl.ds(8 * jb, 8), pl.ds(TILE, TILE)] = low

    build(0, lambda k: coefs[0, k])

    load_tiles.wait()
    pl.semaphore_wait(barrier, len(peers))

    copies = []

    def send(src, dst, peer):
        i = len(copies)
        copy = pltpu.make_async_remote_copy(
            src_ref=src,
            dst_ref=dst,
            send_sem=send_sem.at[i],
            recv_sem=recv_sem.at[i],
            device_id=peer,
            device_id_type=MESH,
        )
        copy.start()
        copies.append(copy)

    for j in range(1, SPAN):
        send(floats.at[0], floats.at[j], (det(j), r))
        send(ints.at[0], ints.at[j], (det(j), r))
    low_rows, high_rows = pl.ds(0, ABOVE), pl.ds(ABOVE + BAND, BELOW)
    for side, j, at in ((0, 1, 6), (1, -1, 9)):
        send(edges.at[side], tiles.at[pl.ds(at, CAP), pl.ds(ABOVE, BAND), :], (det(j), r))
        send(
            edges.at[side, :, pl.ds(0, BELOW), :],
            tiles.at[pl.ds(at, CAP), high_rows, :],
            (det(j), row(-1)),
        )
        send(
            edges.at[side, :, pl.ds(BAND - ABOVE, ABOVE), :],
            tiles.at[pl.ds(at, CAP), low_rows, :],
            (det(j), row(1)),
        )
    send(own.at[:, pl.ds(0, BELOW), :], tiles.at[pl.ds(0, TILES), high_rows, :], (p, row(-1)))
    send(
        own.at[:, pl.ds(BAND - ABOVE, ABOVE), :],
        tiles.at[pl.ds(0, TILES), low_rows, :],
        (p, row(1)),
    )
    for j in range(1, SPAN):
        send(
            science.at[0, :, pl.ds(j * TILE, CAP * TILE)],
            seen.at[j],
            (det(j), r),
        )

    for copy in copies[:6]:
        copy.wait_recv()
    to_float = pltpu.make_async_copy(floats, float_s, local_sem.at[3])
    to_int = pltpu.make_async_copy(ints, int_s, local_sem.at[4])
    to_float.start()
    to_int.start()
    to_float.wait()
    to_int.wait()
    for q in range(1, SPAN):
        build(q, lambda k, q=q: float_s[q, 0, k])
    for copy in copies[6:14]:
        copy.wait_recv()

    eight = lax.broadcasted_iota(jnp.int32, (2 * BAND, TILE), 0)
    wide = lax.broadcasted_iota(jnp.int32, (2 * BAND, TILE), 1)
    line_at = eight + (r * BAND - HALF)
    tail = wide < HALF
    for q in range(SPAN):
        start, length, first = runs[q]
        before = None
        for m in range(CAP + 2):
            c = jnp.clip(start + (m - 1), 0, TILES - 1)
            row_shift = jnp.clip(int_s[q, 0, c], 0, MAXOFF - 1)
            col_shift = int_s[q, 0, 6 + c]
            row_weight, col_weight = float_s[q, 0, 28 + c], float_s[q, 0, 34 + c]
            if m == 0:
                index = 5 + q if q > 0 else ZERO_TILE
            else:
                right = 9 + q if q < SPAN - 1 else ZERO_TILE
                index = jnp.where(
                    m <= length, first + (m - 1), jnp.where(m == length + 1, right, ZERO_TILE)
                )
                index = jnp.clip(index, 0, ZERO_TILE)
            upper = tiles[index, pl.ds(1 + row_shift, 2 * BAND), :]
            lower = tiles[index, pl.ds(2 + row_shift, 2 * BAND), :]
            limit = row_count * BAND - row_shift
            upper = jnp.where(line_at < limit, (1.0 - row_weight) * upper, 0.0)
            lower = jnp.where(line_at < limit - 1, row_weight * lower, 0.0)
            mixed = jnp.where(line_at >= 0, upper + lower, 0.0)
            last = jnp.broadcast_to(mixed[:, TILE - 1 :], (2 * BAND, TILE))
            left = pltpu.roll(mixed, HALF - col_shift, 1)
            left = jnp.where(tail & (wide > HALF - 1 - col_shift), last, left)
            following = pltpu.roll(mixed, HALF - 1 - col_shift, 1)
            following = jnp.where(tail & (wide > HALF - 2 - col_shift), last, following)
            now = (1.0 - col_weight) * left + col_weight * following
            if m > 0:
                high, low = split(jnp.where(tail, before, now))
                images[q, 0, m - 1] = high
                images[q, 1, m - 1] = low
            before = now

    rest = jnp.zeros((2 * TILE - TILE - BAND, 2 * TILE), jnp.float32)
    sums = []
    for pair in range(SPAN // 2):
        accs = [None, None]
        for a in range(KW):
            for i in range(2):
                q = 2 * pair + i
                blocks = []
                for part in range(2):
                    views = [images[q, part, k, pl.ds(a, BAND), :] for k in range(CAP + 1)]
                    blocks += [
                        jnp.concatenate([views[k], views[k + 1]], axis=1) for k in range(CAP)
                    ]
                band = jnp.concatenate([bands[q, a], rest], axis=0)
                term = jnp.dot(
                    jnp.concatenate(blocks, axis=0), band, preferred_element_type=jnp.float32
                )
                accs[i] = term if accs[i] is None else accs[i] + term
        sums += accs

    load_seen.wait()
    for copy in copies[14:]:
        copy.wait_recv()

    down = lax.broadcasted_iota(jnp.int32, (BAND, TILE), 0) + r * BAND
    parts = []
    for q in range(SPAN):
        start, length, first = runs[q]
        for k in range(CAP):
            acc = sums[q]
            at = k * BAND
            model = acc[at : at + BAND, :TILE] + acc[at : at + BAND, TILE:]
            at += CAP * BAND
            model = model + (acc[at : at + BAND, :TILE] + acc[at : at + BAND, TILE:])
            pixels = seen[q, :, pl.ds(k * TILE, TILE)]
            if k == 0 and q > 0:
                pixels = jnp.where(start == q, pixels, seen[q, :, pl.ds(2 * TILE, TILE)])
            c = jnp.clip(start + k, 0, TILES - 1)
            residual = jnp.where(
                down < int_s[q, 0, 12 + c], pixels - model - float_s[q, 0, NB], 0.0
            )
            parts.append((jnp.where(k < length, first + k, -1), residual))
    for s in range(TILES):
        total = jnp.zeros((BAND, TILE), jnp.float32)
        tally = jnp.float32(0.0)
        for slot, residual in parts:
            total = total + jnp.where(slot == s, residual, 0.0)
            tally = tally + jnp.where(slot == s, 1.0, 0.0)
        out[0, s] = total / jnp.maximum(tally, 1.0)

    for copy in copies:
        copy.wait_send()


def solution(mesh):
    det_count, row_count = mesh.shape["det"], mesh.shape["row"]

    def body(
        science, template, sources, offsets, weights, valid, basis, coefs, background
    ):
        smem = pl.BlockSpec(memory_space=pltpu.SMEM)
        vmem = pl.BlockSpec(memory_space=pltpu.VMEM)
        hbm = pl.BlockSpec(memory_space=pl.ANY)
        return pl.pallas_call(
            functools.partial(kernel, det_count, row_count),
            out_shape=jax.ShapeDtypeStruct(template.shape, jnp.float32),
            in_specs=[hbm, hbm, smem, smem, smem, smem, vmem, smem, smem],
            out_specs=vmem,
            scratch_shapes=[
                pltpu.VMEM((TILES, BAND, TILE), jnp.float32),
                pltpu.VMEM((ZERO_TILE + 1, DEEP, TILE), jnp.float32),
                pltpu.VMEM((2, CAP, BAND, TILE), jnp.float32),
                pltpu.VMEM((SPAN, 2, CAP + 1, 2 * BAND, TILE), jnp.float32),
                pltpu.VMEM((SPAN, BAND, CAP * TILE), jnp.float32),
                pltpu.VMEM((SPAN, KW, TILE + BAND, 2 * TILE), jnp.float32),
                pltpu.VMEM((BAND, TILE), jnp.float32),
                pltpu.VMEM((BAND, TILE), jnp.float32),
                pltpu.VMEM((SPAN, 1, TILE), jnp.float32),
                pltpu.VMEM((SPAN, 1, TILE), jnp.int32),
                pltpu.SMEM((SPAN, 1, TILE), jnp.float32),
                pltpu.SMEM((SPAN, 1, TILE), jnp.int32),
                pltpu.SemaphoreType.DMA((5,)),
                pltpu.SemaphoreType.DMA((17,)),
                pltpu.SemaphoreType.DMA((17,)),
            ],
            compiler_params=pltpu.CompilerParams(
                collective_id=0, has_side_effects=True, vmem_limit_bytes=40 << 20
            ),
        )(
            science,
            template,
            sources.T,
            offsets,
            weights,
            valid,
            basis,
            coefs,
            background,
        )

    in_specs = (
        P("det", "row", None),
        P("det", None, "row", None),
        P(),
        P(None, "det", None),
        P(None, "det", None),
        P("det", None),
        P(),
        P("det", None),
        P("det"),
    )
    out_specs = P("det", None, "row", None)
    return jax.shard_map(body, mesh=mesh, in_specs=in_specs, out_specs=out_specs, check_vma=False)
```

```python
import functools

import jax
import jax.numpy as jnp
from jax import lax
from jax.experimental import pallas as pl
from jax.experimental.pallas import tpu as pltpu
from jax.sharding import PartitionSpec as P

MESH = pl.DeviceIdType.MESH
SPAN = 4
CAP = 3
TILES = 6
TILE = 128
BAND = 32
ABOVE = 16
BELOW = 24
DEEP = ABOVE + BAND + BELOW
KW = 31
HALF = 15
NB = 27
GROUP = 8
MAXOFF = 4
STRIP = 32
LEFT, RIGHT, ZERO_TILE = 6, 7, 8


def split(x):
    high = x.astype(jnp.bfloat16).astype(jnp.float32)
    return high, x - high


def kernel(
    det_count,
    row_count,
    science,
    template,
    sources,
    offsets,
    weights,
    valid,
    basis,
    coefs,
    background,
    out,
    tally_out,
    own,
    tiles,
    edges,
    images,
    seen,
    bands_even,
    bands_odd,
    basis_v,
    model_v,
    taps,
    taps_back,
    floats,
    ints,
    float_s,
    int_s,
    sources_s,
    offsets_s,
    weights_s,
    valid_s,
    coefs_s,
    local_sem,
    send_sem,
    recv_sem,
):
    p = lax.axis_index("det")
    r = lax.axis_index("row")

    def det(j):
        return lax.rem(p + (j + det_count), det_count)

    def row(j):
        return lax.rem(r + (j + row_count), row_count)

    peers = [(det(j), r) for j in (1, -1, 2, -2, 3, -3)]
    peers += [(p, row(1)), (p, row(-1))]
    peers += [(det(j), row(i)) for j in (1, -1) for i in (1, -1)]
    barrier = pltpu.get_barrier_semaphore()
    for peer in peers:
        pl.semaphore_signal(barrier, inc=1, device_id=peer, device_id_type=MESH)

    load_own = pltpu.make_async_copy(template.at[0], own, local_sem.at[0])
    load_tiles = pltpu.make_async_copy(
        template.at[0], tiles.at[pl.ds(0, TILES), pl.ds(ABOVE, BAND), :], local_sem.at[1]
    )
    load_seen = pltpu.make_async_copy(
        science.at[0, :, pl.ds(0, CAP * TILE)], seen.at[0], local_sem.at[2]
    )
    load_basis = pltpu.make_async_copy(basis, basis_v, local_sem.at[5])
    small = []
    for i, (src, dst) in enumerate(
        (
            (sources, sources_s),
            (offsets, offsets_s),
            (weights, weights_s),
            (valid, valid_s),
            (coefs, coefs_s),
        )
    ):
        small.append(pltpu.make_async_copy(src, dst, local_sem.at[6 + i]))
    load_own.start()
    for copy in small:
        copy.start()
    load_basis.start()
    load_tiles.start()
    load_seen.start()
    for copy in small:
        copy.wait()

    runs = []
    for q in range(SPAN):
        d = det(-q)
        start = jnp.int32(0)
        length = jnp.int32(0)
        for c in range(TILES):
            reach = lax.rem(sources_s[c, d] // TILES - d + det_count, det_count)
            start = start + jnp.where(reach < q, 1, 0)
            length = length + jnp.where(reach == q, 1, 0)
        start = jnp.clip(start, 0, TILES - 1)
        first = jnp.clip(sources_s[start, d] - p * TILES, 0, TILES - 1)
        runs.append((start, length, first))

    lane = lax.broadcasted_iota(jnp.int32, (1, TILE), 1)
    packed = jnp.zeros((1, TILE), jnp.float32)
    whole = jnp.zeros((1, TILE), jnp.int32)
    for k in range(NB):
        packed = jnp.where(lane == k, coefs_s[0, k], packed)
    packed = jnp.where(lane == NB, background[0], packed)
    for c in range(TILES):
        packed = jnp.where(lane == 28 + c, weights_s[0, 0, c], packed)
        packed = jnp.where(lane == 34 + c, weights_s[1, 0, c], packed)
        whole = jnp.where(lane == c, offsets_s[0, 0, c], whole)
        whole = jnp.where(lane == 6 + c, offsets_s[1, 0, c], whole)
        whole = jnp.where(lane == 12 + c, valid_s[0, c], whole)
    floats[0] = packed
    ints[0] = whole

    tiles[ZERO_TILE] = jnp.zeros((DEEP, TILE), jnp.float32)
    load_own.wait()
    strip = lax.broadcasted_iota(jnp.int32, (BAND, TILE), 1) // STRIP
    ends = jnp.zeros((BAND, TILE), jnp.float32)
    begins = jnp.zeros((BAND, TILE), jnp.float32)
    for j in range(CAP):
        start, length, first = runs[j]
        last = own[jnp.clip(first + length - 1, 0, TILES - 1)]
        ends = jnp.where(strip == j, pltpu.roll(last, STRIP * (j + 1), 1), ends)
        start, length, first = runs[j + 1]
        head = own[first]
        begins = jnp.where(strip == j, pltpu.roll(head, STRIP * j, 1) if j else head, begins)
    edges[0] = ends
    edges[1] = begins

    load_tiles.wait()
    pl.semaphore_wait(barrier, len(peers))

    copies = []

    def send(src, dst, peer):
        i = len(copies)
        copy = pltpu.make_async_remote_copy(
            src_ref=src,
            dst_ref=dst,
            send_sem=send_sem.at[i],
            recv_sem=recv_sem.at[i],
            device_id=peer,
            device_id_type=MESH,
        )
        copy.start()
        copies.append(copy)

    low_rows, high_rows = pl.ds(0, ABOVE), pl.ds(ABOVE + BAND, BELOW)
    send(own.at[:, pl.ds(0, BELOW), :], tiles.at[pl.ds(0, TILES), high_rows, :], (p, row(-1)))
    send(
        own.at[:, pl.ds(BAND - ABOVE, ABOVE), :],
        tiles.at[pl.ds(0, TILES), low_rows, :],
        (p, row(1)),
    )
    for j in range(1, SPAN):
        send(floats.at[0], floats.at[j], (det(j), r))
        send(ints.at[0], ints.at[j], (det(j), r))
    for side, j, at in ((0, 1, LEFT), (1, -1, RIGHT)):
        send(
            edges.at[side, pl.ds(0, BELOW), :], tiles.at[at, high_rows, :], (det(j), row(-1))
        )
        send(
            edges.at[side, pl.ds(BAND - ABOVE, ABOVE), :],
            tiles.at[at, low_rows, :],
            (det(j), row(1)),
        )
        send(edges.at[side], tiles.at[at, pl.ds(ABOVE, BAND), :], (det(j), r))
    for j in range(1, SPAN):
        send(
            science.at[0, :, pl.ds(j * TILE, CAP * TILE)],
            seen.at[j],
            (det(j), r),
        )

    sub = lax.broadcasted_iota(jnp.int32, (8, TILE), 0)
    across = lax.broadcasted_iota(jnp.int32, (8, TILE), 1)

    def mirrored(q, coefficient):
        total = coefficient(0) * basis_v[0]
        for k in range(1, NB):
            total = total + coefficient(k) * basis_v[k]
        taps[pl.ds(0, KW), pl.ds(0, KW)] = total
        high, low = split(taps[...])
        both = jnp.dot(
            jnp.concatenate([high, low], axis=0), mirror, preferred_element_type=jnp.float32
        )
        taps_back[q] = both[:BAND] + both[BAND:]

    def toeplitz(q, a, bands, place):
        line = jnp.broadcast_to(taps_back[q, pl.ds(a, 1), :], (8, TILE))
        block = pltpu.roll(line, 0, 1, stride=1, stride_axis=0)
        for jb in range(TILE // 8):
            high, low = split(block if jb == 0 else pltpu.roll(block, 8 * jb, 1))
            if jb < BAND // 8:
                lead = across <= sub + 8 * jb
                at = pl.ds(TILE + 8 * jb, 8)
                bands[place, a, at, pl.ds(0, TILE)] = jnp.where(lead, 0.0, high)
                bands[place, a, at, pl.ds(TILE, TILE)] = jnp.where(lead, 0.0, low)
                high, low = jnp.where(lead, high, 0.0), jnp.where(lead, low, 0.0)
            bands[place, a, pl.ds(8 * jb, 8), pl.ds(0, TILE)] = high
            bands[place, a, pl.ds(8 * jb, 8), pl.ds(TILE, TILE)] = low

    def toeplitz_first_pair(q):
        def group(step, carry):
            for k in range(GROUP):
                toeplitz(q, step * GROUP + k, bands_even, q)
            return carry

        lax.fori_loop(0, BAND // GROUP, group, 0)

    rows128 = lax.broadcasted_iota(jnp.int32, (TILE, TILE), 0)
    cols128 = lax.broadcasted_iota(jnp.int32, (TILE, TILE), 1)
    mirror = jnp.where(lax.rem(rows128 + cols128, TILE) == 0, 1.0, 0.0).astype(jnp.float32)
    taps[...] = jnp.zeros((BAND, TILE), jnp.float32)
    load_basis.wait()
    mirrored(0, lambda k: coefs_s[0, k])
    toeplitz_first_pair(0)
    for copy in copies[2:8]:
        copy.wait_recv()
    to_float = pltpu.make_async_copy(floats, float_s, local_sem.at[3])
    to_int = pltpu.make_async_copy(ints, int_s, local_sem.at[4])
    to_float.start()
    to_int.start()
    to_float.wait()
    to_int.wait()
    for q in range(1, SPAN):
        mirrored(q, lambda k, q=q: float_s[q, 0, k])
    toeplitz_first_pair(1)
    for copy in copies[:2] + copies[8:14]:
        copy.wait_recv()

    eight = lax.broadcasted_iota(jnp.int32, (2 * BAND, TILE), 0)
    wide = lax.broadcasted_iota(jnp.int32, (2 * BAND, TILE), 1)
    line_at = eight + (r * BAND - HALF)
    tail = wide < HALF
    for q in range(SPAN):
        start, length, first = runs[q]
        before = None
        for m in range(CAP + 2):
            c = jnp.clip(start + (m - 1), 0, TILES - 1)
            row_shift = jnp.clip(int_s[q, 0, c], 0, MAXOFF - 1)
            col_shift = int_s[q, 0, 6 + c]
            row_weight, col_weight = float_s[q, 0, 28 + c], float_s[q, 0, 34 + c]
            turn = jnp.int32(HALF + TILE) - col_shift
            last_lane = TILE - 1
            if m == 0:
                index = LEFT if q > 0 else ZERO_TILE
                last_lane = STRIP * q - 1 if q > 0 else TILE - 1
                turn = turn - STRIP * q
            else:
                edge = RIGHT if q < SPAN - 1 else ZERO_TILE
                index = jnp.where(
                    m <= length, first + (m - 1), jnp.where(m == length + 1, edge, ZERO_TILE)
                )
                index = jnp.clip(index, 0, ZERO_TILE)
                if q > 0:
                    turn = turn - jnp.where(m > length, STRIP * q, 0)
            upper = tiles[index, pl.ds(1 + row_shift, 2 * BAND), :]
            lower = tiles[index, pl.ds(2 + row_shift, 2 * BAND), :]
            limit = row_count * BAND - row_shift
            upper = jnp.where(line_at < limit, (1.0 - row_weight) * upper, 0.0)
            lower = jnp.where(line_at < limit - 1, row_weight * lower, 0.0)
            mixed = jnp.where(line_at >= 0, upper + lower, 0.0)
            last = jnp.broadcast_to(mixed[:, last_lane : last_lane + 1], (2 * BAND, TILE))
            left = pltpu.roll(mixed, lax.rem(turn, TILE), 1)
            left = jnp.where(tail & (wide > HALF - 1 - col_shift), last, left)
            following = pltpu.roll(mixed, lax.rem(turn - 1, TILE), 1)
            following = jnp.where(tail & (wide > HALF - 2 - col_shift), last, following)
            now = (1.0 - col_weight) * left + col_weight * following
            if m > 0:
                high, low = split(jnp.where(tail, before, now))
                images[q, 0, m - 1] = high
                images[q, 1, m - 1] = low
            before = now

    rest = jnp.zeros((TILE - BAND, 2 * TILE), jnp.float32)
    model_v[...] = jnp.zeros_like(model_v)

    def convolve(pair, bands):
        def group(step, carry):
            base = step * GROUP
            for i in range(2):
                q = 2 * pair + i
                if pair == 0:
                    for k in range(GROUP):
                        toeplitz(q + 2, base + k, bands_odd, i)
                total = None
                for k in range(GROUP):
                    blocks = []
                    for part in range(2):
                        views = [
                            images[q, part, t, pl.ds(base + k, BAND), :] for t in range(CAP + 1)
                        ]
                        blocks += [
                            jnp.concatenate([views[t], views[t + 1]], axis=1)
                            for t in range(CAP)
                        ]
                    band = jnp.concatenate([bands[i, base + k], rest], axis=0)
                    term = jnp.dot(
                        jnp.concatenate(blocks, axis=0), band, preferred_element_type=jnp.float32
                    )
                    total = term if total is None else total + term
                model_v[q] += total
            return carry

        lax.fori_loop(0, BAND // GROUP, group, 0)

    convolve(0, bands_even)
    convolve(1, bands_odd)

    load_seen.wait()
    for copy in copies[14:]:
        copy.wait_recv()

    down = lax.broadcasted_iota(jnp.int32, (BAND, TILE), 0) + r * BAND
    parts = []
    for q in range(SPAN):
        start, length, first = runs[q]
        for k in range(CAP):
            acc = model_v[q]
            at = k * BAND
            model = acc[at : at + BAND, :TILE] + acc[at : at + BAND, TILE:]
            at += CAP * BAND
            model = model + (acc[at : at + BAND, :TILE] + acc[at : at + BAND, TILE:])
            pixels = seen[q, :, pl.ds(k * TILE, TILE)]
            if k == 0 and q > 0:
                pixels = jnp.where(start == q, pixels, seen[q, :, pl.ds(2 * TILE, TILE)])
            c = jnp.clip(start + k, 0, TILES - 1)
            residual = jnp.where(
                down < int_s[q, 0, 12 + c], pixels - model - float_s[q, 0, NB], 0.0
            )
            parts.append((jnp.where(k < length, first + k, -1), residual))
    for s in range(TILES):
        total = jnp.zeros((BAND, TILE), jnp.float32)
        tally = jnp.float32(0.0)
        for slot, residual in parts:
            total = total + jnp.where(slot == s, residual, 0.0)
            tally = tally + jnp.where(slot == s, 1.0, 0.0)
        out[0, s] = total
        tally_out[0, s] = jnp.full((BAND, TILE), jnp.maximum(tally, 1.0), jnp.float32)

    for copy in copies:
        copy.wait_send()


def solution(mesh):
    det_count, row_count = mesh.shape["det"], mesh.shape["row"]

    def body(
        science, template, sources, offsets, weights, valid, basis, coefs, background
    ):
        vmem = pl.BlockSpec(memory_space=pltpu.VMEM)
        hbm = pl.BlockSpec(memory_space=pltpu.HBM)
        total, tally = pl.pallas_call(
            functools.partial(kernel, det_count, row_count),
            out_shape=(
                jax.ShapeDtypeStruct(template.shape, jnp.float32),
                jax.ShapeDtypeStruct(template.shape, jnp.float32),
            ),
            in_specs=[hbm] * 8 + [pl.BlockSpec(memory_space=pltpu.SMEM)],
            out_specs=(vmem, vmem),
            scratch_shapes=[
                pltpu.VMEM((TILES, BAND, TILE), jnp.float32),
                pltpu.VMEM((ZERO_TILE + 1, DEEP, TILE), jnp.float32),
                pltpu.VMEM((2, BAND, TILE), jnp.float32),
                pltpu.VMEM((SPAN, 2, CAP + 1, 2 * BAND, TILE), jnp.float32),
                pltpu.VMEM((SPAN, BAND, CAP * TILE), jnp.float32),
                pltpu.VMEM((2, BAND, TILE + BAND, 2 * TILE), jnp.float32),
                pltpu.VMEM((2, BAND, TILE + BAND, 2 * TILE), jnp.float32),
                pltpu.VMEM((NB, KW, KW), jnp.float32),
                pltpu.VMEM((SPAN, 2 * CAP * BAND, 2 * TILE), jnp.float32),
                pltpu.VMEM((BAND, TILE), jnp.float32),
                pltpu.VMEM((SPAN, BAND, TILE), jnp.float32),
                pltpu.VMEM((SPAN, 1, TILE), jnp.float32),
                pltpu.VMEM((SPAN, 1, TILE), jnp.int32),
                pltpu.SMEM((SPAN, 1, TILE), jnp.float32),
                pltpu.SMEM((SPAN, 1, TILE), jnp.int32),
                pltpu.SMEM((TILES, TILE), jnp.int32),
                pltpu.SMEM((2, 1, TILES), jnp.int32),
                pltpu.SMEM((2, 1, TILES), jnp.float32),
                pltpu.SMEM((1, TILES), jnp.int32),
                pltpu.SMEM((1, NB), jnp.float32),
                pltpu.SemaphoreType.DMA((11,)),
                pltpu.SemaphoreType.DMA((17,)),
                pltpu.SemaphoreType.DMA((17,)),
            ],
            compiler_params=pltpu.CompilerParams(
                collective_id=0, has_side_effects=True, vmem_limit_bytes=54 << 20
            ),
        )(
            science,
            template,
            sources.T,
            offsets,
            weights,
            valid,
            basis,
            coefs,
            background,
        )
        return total / tally

    in_specs = (
        P("det", "row", None),
        P("det", None, "row", None),
        P(),
        P(None, "det", None),
        P(None, "det", None),
        P("det", None),
        P(),
        P("det", None),
        P("det"),
    )
    out_specs = P("det", None, "row", None)
    return jax.shard_map(body, mesh=mesh, in_specs=in_specs, out_specs=out_specs, check_vma=False)
```

```python
import functools

import jax
import jax.numpy as jnp
from jax import lax
from jax.experimental import pallas as pl
from jax.experimental.pallas import tpu as pltpu
from jax.sharding import PartitionSpec as P

MESH = pl.DeviceIdType.MESH
SPAN = 4
CAP = 3
TILES = 6
TILE = 128
BAND = 32
ABOVE = 16
BELOW = 24
DEEP = ABOVE + BAND + BELOW
KW = 31
HALF = 15
NB = 27
GROUP = 8
DOTS = 32
MAXOFF = 4
STRIP = 32
LEFT, RIGHT, ZERO_TILE = 6, 7, 8


def split(x):
    high = x.astype(jnp.bfloat16).astype(jnp.float32)
    return high, x - high


def kernel(
    det_count,
    row_count,
    science,
    template,
    sources,
    offsets,
    weights,
    valid,
    basis,
    coefs,
    background,
    out,
    tally_out,
    own,
    tiles,
    edges,
    images,
    seen,
    bands_even,
    bands_odd,
    basis_v,
    model_v,
    taps,
    taps_back,
    floats,
    ints,
    float_s,
    int_s,
    sources_s,
    offsets_s,
    weights_s,
    valid_s,
    coefs_s,
    local_sem,
    send_sem,
    recv_sem,
):
    p = lax.axis_index("det")
    r = lax.axis_index("row")

    def det(j):
        return lax.rem(p + (j + det_count), det_count)

    def row(j):
        return lax.rem(r + (j + row_count), row_count)

    peers = [(det(j), r) for j in (1, -1, 2, -2, 3, -3)]
    peers += [(p, row(1)), (p, row(-1))]
    peers += [(det(j), row(i)) for j in (1, -1) for i in (1, -1)]
    barrier = pltpu.get_barrier_semaphore()
    for peer in peers:
        pl.semaphore_signal(barrier, inc=1, device_id=peer, device_id_type=MESH)

    load_own = pltpu.make_async_copy(template.at[0], own, local_sem.at[0])
    load_tiles = pltpu.make_async_copy(
        template.at[0], tiles.at[pl.ds(0, TILES), pl.ds(ABOVE, BAND), :], local_sem.at[1]
    )
    load_seen = pltpu.make_async_copy(
        science.at[0, :, pl.ds(0, CAP * TILE)], seen.at[0], local_sem.at[2]
    )
    load_basis = pltpu.make_async_copy(basis, basis_v, local_sem.at[5])
    small = []
    for i, (src, dst) in enumerate(
        (
            (sources, sources_s),
            (offsets, offsets_s),
            (weights, weights_s),
            (valid, valid_s),
            (coefs, coefs_s),
        )
    ):
        small.append(pltpu.make_async_copy(src, dst, local_sem.at[6 + i]))
    load_own.start()
    for copy in small:
        copy.start()
    load_basis.start()
    load_tiles.start()
    load_seen.start()
    for copy in small:
        copy.wait()

    lane = lax.broadcasted_iota(jnp.int32, (1, TILE), 1)
    packed = jnp.zeros((1, TILE), jnp.float32)
    whole = jnp.zeros((1, TILE), jnp.int32)
    for k in range(NB):
        packed = jnp.where(lane == k, coefs_s[0, k], packed)
    packed = jnp.where(lane == NB, background[0], packed)
    for c in range(TILES):
        packed = jnp.where(lane == 28 + c, weights_s[0, 0, c], packed)
        packed = jnp.where(lane == 34 + c, weights_s[1, 0, c], packed)
        whole = jnp.where(lane == c, offsets_s[0, 0, c], whole)
        whole = jnp.where(lane == 6 + c, offsets_s[1, 0, c], whole)
        whole = jnp.where(lane == 12 + c, valid_s[0, c], whole)
    floats[0] = packed
    ints[0] = whole

    load_own.wait()
    pl.semaphore_wait(barrier, len(peers))

    copies = []

    def send(src, dst, peer):
        i = len(copies)
        copy = pltpu.make_async_remote_copy(
            src_ref=src,
            dst_ref=dst,
            send_sem=send_sem.at[i],
            recv_sem=recv_sem.at[i],
            device_id=peer,
            device_id_type=MESH,
        )
        copy.start()
        copies.append(copy)

    low_rows, high_rows = pl.ds(0, ABOVE), pl.ds(ABOVE + BAND, BELOW)
    send(own.at[:, pl.ds(0, BELOW), :], tiles.at[pl.ds(0, TILES), high_rows, :], (p, row(-1)))
    send(
        own.at[:, pl.ds(BAND - ABOVE, ABOVE), :],
        tiles.at[pl.ds(0, TILES), low_rows, :],
        (p, row(1)),
    )
    for j in range(1, SPAN):
        send(floats.at[0], floats.at[j], (det(j), r))
        send(ints.at[0], ints.at[j], (det(j), r))

    runs = []
    for q in range(SPAN):
        d = det(-q)
        start = jnp.int32(0)
        length = jnp.int32(0)
        for c in range(TILES):
            reach = lax.rem(sources_s[c, d] // TILES - d + det_count, det_count)
            start = start + jnp.where(reach < q, 1, 0)
            length = length + jnp.where(reach == q, 1, 0)
        start = jnp.clip(start, 0, TILES - 1)
        first = jnp.clip(sources_s[start, d] - p * TILES, 0, TILES - 1)
        runs.append((start, length, first))

    tiles[ZERO_TILE] = jnp.zeros((DEEP, TILE), jnp.float32)
    strip = lax.broadcasted_iota(jnp.int32, (BAND, TILE), 1) // STRIP
    ends = jnp.zeros((BAND, TILE), jnp.float32)
    begins = jnp.zeros((BAND, TILE), jnp.float32)
    for j in range(CAP):
        start, length, first = runs[j]
        last = own[jnp.clip(first + length - 1, 0, TILES - 1)]
        ends = jnp.where(strip == j, pltpu.roll(last, STRIP * (j + 1), 1), ends)
        start, length, first = runs[j + 1]
        head = own[first]
        begins = jnp.where(strip == j, pltpu.roll(head, STRIP * j, 1) if j else head, begins)
    edges[0] = ends
    edges[1] = begins

    for side, j, at in ((0, 1, LEFT), (1, -1, RIGHT)):
        send(
            edges.at[side, pl.ds(0, BELOW), :], tiles.at[at, high_rows, :], (det(j), row(-1))
        )
        send(
            edges.at[side, pl.ds(BAND - ABOVE, ABOVE), :],
            tiles.at[at, low_rows, :],
            (det(j), row(1)),
        )
        send(edges.at[side], tiles.at[at, pl.ds(ABOVE, BAND), :], (det(j), r))
    for j in range(1, SPAN):
        send(
            science.at[0, :, pl.ds(j * TILE, CAP * TILE)],
            seen.at[j],
            (det(j), r),
        )

    sub = lax.broadcasted_iota(jnp.int32, (8, TILE), 0)
    across = lax.broadcasted_iota(jnp.int32, (8, TILE), 1)

    def mirrored(q, coefficient):
        total = coefficient(0) * basis_v[0]
        for k in range(1, NB):
            total = total + coefficient(k) * basis_v[k]
        taps[pl.ds(0, KW), pl.ds(0, KW)] = total
        high, low = split(taps[...])
        both = jnp.dot(
            jnp.concatenate([high, low], axis=0), mirror, preferred_element_type=jnp.float32
        )
        taps_back[q] = both[:BAND] + both[BAND:]

    def toeplitz(q, a, bands, place):
        line = jnp.broadcast_to(taps_back[q, pl.ds(a, 1), :], (8, TILE))
        block = pltpu.roll(line, 0, 1, stride=1, stride_axis=0)
        for jb in range(TILE // 8):
            high, low = split(block if jb == 0 else pltpu.roll(block, 8 * jb, 1))
            if jb < BAND // 8:
                lead = across <= sub + 8 * jb
                at = pl.ds(TILE + 8 * jb, 8)
                bands[place, a, at, pl.ds(0, TILE)] = jnp.where(lead, 0.0, high)
                bands[place, a, at, pl.ds(TILE, TILE)] = jnp.where(lead, 0.0, low)
                high, low = jnp.where(lead, high, 0.0), jnp.where(lead, low, 0.0)
            bands[place, a, pl.ds(8 * jb, 8), pl.ds(0, TILE)] = high
            bands[place, a, pl.ds(8 * jb, 8), pl.ds(TILE, TILE)] = low

    def toeplitz_first_pair(q):
        def group(step, carry):
            for k in range(GROUP):
                toeplitz(q, step * GROUP + k, bands_even, q)
            return carry

        lax.fori_loop(0, BAND // GROUP, group, 0)

    rows128 = lax.broadcasted_iota(jnp.int32, (TILE, TILE), 0)
    cols128 = lax.broadcasted_iota(jnp.int32, (TILE, TILE), 1)
    mirror = jnp.where(lax.rem(rows128 + cols128, TILE) == 0, 1.0, 0.0).astype(jnp.float32)
    taps[...] = jnp.zeros((BAND, TILE), jnp.float32)
    load_basis.wait()
    mirrored(0, lambda k: coefs_s[0, k])
    toeplitz_first_pair(0)
    for copy in copies[2:8]:
        copy.wait_recv()
    to_float = pltpu.make_async_copy(floats, float_s, local_sem.at[3])
    to_int = pltpu.make_async_copy(ints, int_s, local_sem.at[4])
    to_float.start()
    to_int.start()
    to_float.wait()
    to_int.wait()
    for q in range(1, SPAN):
        mirrored(q, lambda k, q=q: float_s[q, 0, k])
    toeplitz_first_pair(1)
    load_tiles.wait()
    for copy in copies[:2] + copies[8:14]:
        copy.wait_recv()

    eight = lax.broadcasted_iota(jnp.int32, (2 * BAND, TILE), 0)
    wide = lax.broadcasted_iota(jnp.int32, (2 * BAND, TILE), 1)
    line_at = eight + (r * BAND - HALF)
    tail = wide < HALF
    for q in range(SPAN):
        start, length, first = runs[q]
        before = None
        for m in range(CAP + 2):
            c = jnp.clip(start + (m - 1), 0, TILES - 1)
            row_shift = jnp.clip(int_s[q, 0, c], 0, MAXOFF - 1)
            col_shift = int_s[q, 0, 6 + c]
            row_weight, col_weight = float_s[q, 0, 28 + c], float_s[q, 0, 34 + c]
            turn = jnp.int32(HALF + TILE) - col_shift
            last_lane = TILE - 1
            if m == 0:
                index = LEFT if q > 0 else ZERO_TILE
                last_lane = STRIP * q - 1 if q > 0 else TILE - 1
                turn = turn - STRIP * q
            else:
                edge = RIGHT if q < SPAN - 1 else ZERO_TILE
                index = jnp.where(
                    m <= length, first + (m - 1), jnp.where(m == length + 1, edge, ZERO_TILE)
                )
                index = jnp.clip(index, 0, ZERO_TILE)
                if q > 0:
                    turn = turn - jnp.where(m > length, STRIP * q, 0)
            upper = tiles[index, pl.ds(1 + row_shift, 2 * BAND), :]
            lower = tiles[index, pl.ds(2 + row_shift, 2 * BAND), :]
            limit = row_count * BAND - row_shift
            upper = jnp.where(line_at < limit, (1.0 - row_weight) * upper, 0.0)
            lower = jnp.where(line_at < limit - 1, row_weight * lower, 0.0)
            mixed = jnp.where(line_at >= 0, upper + lower, 0.0)
            last = jnp.broadcast_to(mixed[:, last_lane : last_lane + 1], (2 * BAND, TILE))
            left = pltpu.roll(mixed, lax.rem(turn, TILE), 1)
            left = jnp.where(tail & (wide > HALF - 1 - col_shift), last, left)
            following = pltpu.roll(mixed, lax.rem(turn - 1, TILE), 1)
            following = jnp.where(tail & (wide > HALF - 2 - col_shift), last, following)
            now = (1.0 - col_weight) * left + col_weight * following
            if m > 0:
                high, low = split(jnp.where(tail, before, now))
                images[q, 0, m - 1] = high
                images[q, 1, m - 1] = low
            before = now

    rest = jnp.zeros((TILE - BAND, 2 * TILE), jnp.float32)
    model_v[...] = jnp.zeros_like(model_v)

    def convolve(pair, bands):
        def group(step, carry):
            base = step * DOTS
            for i in range(2):
                q = 2 * pair + i
                if pair == 0:
                    for k in range(DOTS):
                        toeplitz(q + 2, base + k, bands_odd, i)
                total = None
                for k in range(DOTS):
                    blocks = []
                    for part in range(2):
                        views = [
                            images[q, part, t, pl.ds(base + k, BAND), :] for t in range(CAP + 1)
                        ]
                        blocks += [
                            jnp.concatenate([views[t], views[t + 1]], axis=1)
                            for t in range(CAP)
                        ]
                    band = jnp.concatenate([bands[i, base + k], rest], axis=0)
                    term = jnp.dot(
                        jnp.concatenate(blocks, axis=0), band, preferred_element_type=jnp.float32
                    )
                    total = term if total is None else total + term
                model_v[q] += total
            return carry

        lax.fori_loop(0, BAND // DOTS, group, 0)

    convolve(0, bands_even)
    convolve(1, bands_odd)

    load_seen.wait()
    for copy in copies[14:]:
        copy.wait_recv()

    down = lax.broadcasted_iota(jnp.int32, (BAND, TILE), 0) + r * BAND
    parts = []
    for q in range(SPAN):
        start, length, first = runs[q]
        for k in range(CAP):
            acc = model_v[q]
            at = k * BAND
            model = acc[at : at + BAND, :TILE] + acc[at : at + BAND, TILE:]
            at += CAP * BAND
            model = model + (acc[at : at + BAND, :TILE] + acc[at : at + BAND, TILE:])
            pixels = seen[q, :, pl.ds(k * TILE, TILE)]
            if k == 0 and q > 0:
                pixels = jnp.where(start == q, pixels, seen[q, :, pl.ds(2 * TILE, TILE)])
            c = jnp.clip(start + k, 0, TILES - 1)
            residual = jnp.where(
                down < int_s[q, 0, 12 + c], pixels - model - float_s[q, 0, NB], 0.0
            )
            parts.append((jnp.where(k < length, first + k, -1), residual))
    for s in range(TILES):
        total = jnp.zeros((BAND, TILE), jnp.float32)
        tally = jnp.float32(0.0)
        for slot, residual in parts:
            total = total + jnp.where(slot == s, residual, 0.0)
            tally = tally + jnp.where(slot == s, 1.0, 0.0)
        out[0, s] = total
        tally_out[0, s] = jnp.full((BAND, TILE), jnp.maximum(tally, 1.0), jnp.float32)

    for copy in copies:
        copy.wait_send()


def solution(mesh):
    det_count, row_count = mesh.shape["det"], mesh.shape["row"]

    def body(
        science, template, sources, offsets, weights, valid, basis, coefs, background
    ):
        vmem = pl.BlockSpec(memory_space=pltpu.VMEM)
        hbm = pl.BlockSpec(memory_space=pltpu.HBM)
        total, tally = pl.pallas_call(
            functools.partial(kernel, det_count, row_count),
            out_shape=(
                jax.ShapeDtypeStruct(template.shape, jnp.float32),
                jax.ShapeDtypeStruct(template.shape, jnp.float32),
            ),
            in_specs=[hbm] * 8 + [pl.BlockSpec(memory_space=pltpu.SMEM)],
            out_specs=(vmem, vmem),
            scratch_shapes=[
                pltpu.VMEM((TILES, BAND, TILE), jnp.float32),
                pltpu.VMEM((ZERO_TILE + 1, DEEP, TILE), jnp.float32),
                pltpu.VMEM((2, BAND, TILE), jnp.float32),
                pltpu.VMEM((SPAN, 2, CAP + 1, 2 * BAND, TILE), jnp.float32),
                pltpu.VMEM((SPAN, BAND, CAP * TILE), jnp.float32),
                pltpu.VMEM((2, BAND, TILE + BAND, 2 * TILE), jnp.float32),
                pltpu.VMEM((2, BAND, TILE + BAND, 2 * TILE), jnp.float32),
                pltpu.VMEM((NB, KW, KW), jnp.float32),
                pltpu.VMEM((SPAN, 2 * CAP * BAND, 2 * TILE), jnp.float32),
                pltpu.VMEM((BAND, TILE), jnp.float32),
                pltpu.VMEM((SPAN, BAND, TILE), jnp.float32),
                pltpu.VMEM((SPAN, 1, TILE), jnp.float32),
                pltpu.VMEM((SPAN, 1, TILE), jnp.int32),
                pltpu.SMEM((SPAN, 1, TILE), jnp.float32),
                pltpu.SMEM((SPAN, 1, TILE), jnp.int32),
                pltpu.SMEM((TILES, TILE), jnp.int32),
                pltpu.SMEM((2, 1, TILES), jnp.int32),
                pltpu.SMEM((2, 1, TILES), jnp.float32),
                pltpu.SMEM((1, TILES), jnp.int32),
                pltpu.SMEM((1, NB), jnp.float32),
                pltpu.SemaphoreType.DMA((11,)),
                pltpu.SemaphoreType.DMA((17,)),
                pltpu.SemaphoreType.DMA((17,)),
            ],
            compiler_params=pltpu.CompilerParams(
                collective_id=0, has_side_effects=True, vmem_limit_bytes=54 << 20
            ),
        )(
            science,
            template,
            sources.T,
            offsets,
            weights,
            valid,
            basis,
            coefs,
            background,
        )
        return total / tally

    in_specs = (
        P("det", "row", None),
        P("det", None, "row", None),
        P(),
        P(None, "det", None),
        P(None, "det", None),
        P("det", None),
        P(),
        P("det", None),
        P("det"),
    )
    out_specs = P("det", None, "row", None)
    return jax.shard_map(body, mesh=mesh, in_specs=in_specs, out_specs=out_specs, check_vma=False)
```

```python
import functools

import jax
import jax.numpy as jnp
from jax import lax
from jax.experimental import pallas as pl
from jax.experimental.pallas import tpu as pltpu
from jax.sharding import PartitionSpec as P

MESH = pl.DeviceIdType.MESH
SPAN = 4
CAP = 3
TILES = 6
TILE = 128
BAND = 32
ABOVE = 16
BELOW = 24
DEEP = ABOVE + BAND + BELOW
KW = 31
HALF = 15
NB = 27
GROUP = 8
DOTS = 32
MAXOFF = 4
STEP = 96
STRIP = 32
LEFT, RIGHT, ZERO_TILE = 6, 7, 8


def split(x):
    high = x.astype(jnp.bfloat16).astype(jnp.float32)
    return high, x - high


def kernel(
    det_count,
    row_count,
    science,
    template,
    sources,
    offsets,
    weights,
    valid,
    basis,
    coefs,
    background,
    out,
    tally_out,
    own,
    tiles,
    edges,
    images,
    seen,
    bands_even,
    bands_odd,
    basis_v,
    model_v,
    taps,
    taps_back,
    floats,
    ints,
    float_s,
    int_s,
    sources_s,
    offsets_s,
    weights_s,
    valid_s,
    coefs_s,
    local_sem,
    send_sem,
    recv_sem,
):
    p = lax.axis_index("det")
    r = lax.axis_index("row")

    def det(j):
        return lax.rem(p + (j + det_count), det_count)

    def row(j):
        return lax.rem(r + (j + row_count), row_count)

    peers = [(det(j), r) for j in (1, -1, 2, -2, 3, -3)]
    peers += [(p, row(1)), (p, row(-1))]
    peers += [(det(j), row(i)) for j in (1, -1) for i in (1, -1)]
    barrier = pltpu.get_barrier_semaphore()
    for peer in peers:
        pl.semaphore_signal(barrier, inc=1, device_id=peer, device_id_type=MESH)

    load_own = pltpu.make_async_copy(template.at[0], own, local_sem.at[0])
    load_tiles = pltpu.make_async_copy(
        template.at[0], tiles.at[pl.ds(0, TILES), pl.ds(ABOVE, BAND), :], local_sem.at[1]
    )
    load_seen = pltpu.make_async_copy(
        science.at[0, :, pl.ds(0, CAP * TILE)], seen.at[0], local_sem.at[2]
    )
    load_basis = pltpu.make_async_copy(basis, basis_v, local_sem.at[5])
    small = []
    for i, (src, dst) in enumerate(
        (
            (sources, sources_s),
            (offsets, offsets_s),
            (weights, weights_s),
            (valid, valid_s),
            (coefs, coefs_s),
        )
    ):
        small.append(pltpu.make_async_copy(src, dst, local_sem.at[6 + i]))
    load_own.start()
    for copy in small:
        copy.start()
    load_basis.start()
    load_tiles.start()
    load_seen.start()
    for copy in small:
        copy.wait()

    lane = lax.broadcasted_iota(jnp.int32, (1, TILE), 1)
    packed = jnp.zeros((1, TILE), jnp.float32)
    whole = jnp.zeros((1, TILE), jnp.int32)
    for k in range(NB):
        packed = jnp.where(lane == k, coefs_s[0, k], packed)
    packed = jnp.where(lane == NB, background[0], packed)
    for c in range(TILES):
        packed = jnp.where(lane == 28 + c, weights_s[0, 0, c], packed)
        packed = jnp.where(lane == 34 + c, weights_s[1, 0, c], packed)
        whole = jnp.where(lane == c, offsets_s[0, 0, c], whole)
        whole = jnp.where(lane == 6 + c, offsets_s[1, 0, c], whole)
        whole = jnp.where(lane == 12 + c, valid_s[0, c], whole)
    floats[0] = packed
    ints[0] = whole

    load_own.wait()
    pl.semaphore_wait(barrier, len(peers))

    copies = []

    def send(src, dst, peer):
        i = len(copies)
        copy = pltpu.make_async_remote_copy(
            src_ref=src,
            dst_ref=dst,
            send_sem=send_sem.at[i],
            recv_sem=recv_sem.at[i],
            device_id=peer,
            device_id_type=MESH,
        )
        copy.start()
        copies.append(copy)

    low_rows, high_rows = pl.ds(0, ABOVE), pl.ds(ABOVE + BAND, BELOW)
    send(own.at[:, pl.ds(0, BELOW), :], tiles.at[pl.ds(0, TILES), high_rows, :], (p, row(-1)))
    send(
        own.at[:, pl.ds(BAND - ABOVE, ABOVE), :],
        tiles.at[pl.ds(0, TILES), low_rows, :],
        (p, row(1)),
    )
    for j in range(1, SPAN):
        send(floats.at[0], floats.at[j], (det(j), r))
        send(ints.at[0], ints.at[j], (det(j), r))

    runs = []
    for q in range(SPAN):
        d = det(-q)
        start = jnp.int32(0)
        length = jnp.int32(0)
        for c in range(TILES):
            reach = lax.rem(sources_s[c, d] // TILES - d + det_count, det_count)
            start = start + jnp.where(reach < q, 1, 0)
            length = length + jnp.where(reach == q, 1, 0)
        start = jnp.clip(start, 0, TILES - 1)
        first = jnp.clip(sources_s[start, d] - p * TILES, 0, TILES - 1)
        runs.append((start, length, first))

    tiles[ZERO_TILE] = jnp.zeros((DEEP, TILE), jnp.float32)
    strip = lax.broadcasted_iota(jnp.int32, (BAND, TILE), 1) // STRIP
    ends = jnp.zeros((BAND, TILE), jnp.float32)
    begins = jnp.zeros((BAND, TILE), jnp.float32)
    for j in range(CAP):
        start, length, first = runs[j]
        last = own[jnp.clip(first + length - 1, 0, TILES - 1)]
        ends = jnp.where(strip == j, pltpu.roll(last, STRIP * (j + 1), 1), ends)
        start, length, first = runs[j + 1]
        head = own[first]
        begins = jnp.where(strip == j, pltpu.roll(head, STRIP * j, 1) if j else head, begins)
    edges[0] = ends
    edges[1] = begins

    for side, j, at in ((0, 1, LEFT), (1, -1, RIGHT)):
        send(
            edges.at[side, pl.ds(0, BELOW), :], tiles.at[at, high_rows, :], (det(j), row(-1))
        )
        send(
            edges.at[side, pl.ds(BAND - ABOVE, ABOVE), :],
            tiles.at[at, low_rows, :],
            (det(j), row(1)),
        )
        send(edges.at[side], tiles.at[at, pl.ds(ABOVE, BAND), :], (det(j), r))
    for j in range(1, SPAN):
        send(
            science.at[0, :, pl.ds(j * TILE, CAP * TILE)],
            seen.at[j],
            (det(j), r),
        )


    def mirrored(q, coefficient):
        total = coefficient(0) * basis_v[0]
        for k in range(1, NB):
            total = total + coefficient(k) * basis_v[k]
        taps[pl.ds(0, KW), pl.ds(0, KW)] = total
        high, low = split(taps[...])
        both = jnp.dot(
            jnp.concatenate([high, low], axis=0), mirror, preferred_element_type=jnp.float32
        )
        taps_back[q] = both[:BAND] + both[BAND:]

    def toeplitz(q, a, bands, place):
        line = jnp.broadcast_to(taps_back[q, pl.ds(a, 1), :], (8, TILE))
        block = pltpu.roll(line, 0, 1, stride=1, stride_axis=0)
        for jb in range(TILE // 16):
            turned = jnp.concatenate(
                [
                    block if shift == 0 else pltpu.roll(block, shift, 1)
                    for shift in (16 * jb, 16 * jb + 8)
                ],
                axis=0,
            )
            high = turned.astype(jnp.bfloat16)
            low = (turned - high.astype(jnp.float32)).astype(jnp.bfloat16)
            bands[place, a, pl.ds(16 * jb, 16), pl.ds(0, TILE)] = high
            bands[place, a, pl.ds(16 * jb, 16), pl.ds(TILE, TILE)] = low

    def toeplitz_first_pair(q):
        def group(step, carry):
            for k in range(GROUP):
                toeplitz(q, step * GROUP + k, bands_even, q)
            return carry

        lax.fori_loop(0, BAND // GROUP, group, 0)

    rows128 = lax.broadcasted_iota(jnp.int32, (TILE, TILE), 0)
    cols128 = lax.broadcasted_iota(jnp.int32, (TILE, TILE), 1)
    mirror = jnp.where(lax.rem(rows128 + cols128, TILE) == 0, 1.0, 0.0).astype(jnp.float32)
    taps[...] = jnp.zeros((BAND, TILE), jnp.float32)
    load_basis.wait()
    mirrored(0, lambda k: coefs_s[0, k])
    toeplitz_first_pair(0)
    for copy in copies[2:8]:
        copy.wait_recv()
    to_float = pltpu.make_async_copy(floats, float_s, local_sem.at[3])
    to_int = pltpu.make_async_copy(ints, int_s, local_sem.at[4])
    to_float.start()
    to_int.start()
    to_float.wait()
    to_int.wait()
    for q in range(1, SPAN):
        mirrored(q, lambda k, q=q: float_s[q, 0, k])
    toeplitz_first_pair(1)
    load_tiles.wait()
    for copy in copies[:2] + copies[8:14]:
        copy.wait_recv()

    eight = lax.broadcasted_iota(jnp.int32, (2 * BAND, TILE), 0)
    wide = lax.broadcasted_iota(jnp.int32, (2 * BAND, TILE), 1)
    line_at = eight + (r * BAND - HALF)
    tail = wide < HALF
    for q in range(SPAN):
        start, length, first = runs[q]
        before = former = None
        for m in range(CAP + 2):
            c = jnp.clip(start + (m - 1), 0, TILES - 1)
            row_shift = jnp.clip(int_s[q, 0, c], 0, MAXOFF - 1)
            col_shift = int_s[q, 0, 6 + c]
            row_weight, col_weight = float_s[q, 0, 28 + c], float_s[q, 0, 34 + c]
            turn = jnp.int32(HALF + TILE) - col_shift
            last_lane = TILE - 1
            if m == 0:
                index = LEFT if q > 0 else ZERO_TILE
                last_lane = STRIP * q - 1 if q > 0 else TILE - 1
                turn = turn - STRIP * q
            else:
                edge = RIGHT if q < SPAN - 1 else ZERO_TILE
                index = jnp.where(
                    m <= length, first + (m - 1), jnp.where(m == length + 1, edge, ZERO_TILE)
                )
                index = jnp.clip(index, 0, ZERO_TILE)
                if q > 0:
                    turn = turn - jnp.where(m > length, STRIP * q, 0)
            upper = tiles[index, pl.ds(1 + row_shift, 2 * BAND), :]
            lower = tiles[index, pl.ds(2 + row_shift, 2 * BAND), :]
            limit = row_count * BAND - row_shift
            upper = jnp.where(line_at < limit, (1.0 - row_weight) * upper, 0.0)
            lower = jnp.where(line_at < limit - 1, row_weight * lower, 0.0)
            mixed = jnp.where(line_at >= 0, upper + lower, 0.0)
            last = jnp.broadcast_to(mixed[:, last_lane : last_lane + 1], (2 * BAND, TILE))
            left = pltpu.roll(mixed, lax.rem(turn, TILE), 1)
            left = jnp.where(tail & (wide > HALF - 1 - col_shift), last, left)
            following = pltpu.roll(mixed, lax.rem(turn - 1, TILE), 1)
            following = jnp.where(tail & (wide > HALF - 2 - col_shift), last, following)
            now = (1.0 - col_weight) * left + col_weight * following
            if m > 0:
                t = m - 1
                here = jnp.where(tail, before, now)
                window = here
                if t > 0:
                    skip = TILE - STEP
                    window = jnp.where(wide >= TILE - skip * t, former, here)
                    window = pltpu.roll(window, skip * t, 1)
                high, low = split(window)
                images[q, 0, t] = high
                images[q, 1, t] = low
                former = here
            before = now

    rest = jnp.zeros((TILE, TILE), jnp.bfloat16)
    model_v[...] = jnp.zeros_like(model_v)

    def convolve(pair, bands):
        def group(step, carry):
            base = step * DOTS
            for i in range(2):
                q = 2 * pair + i
                if pair == 0:
                    for k in range(DOTS):
                        toeplitz(q + 2, base + k, bands_odd, i)
                total = None
                for k in range(DOTS):
                    blocks = [
                        jnp.concatenate(
                            [images[q, part, t, pl.ds(base + k, BAND), :] for part in range(2)],
                            axis=1,
                        )
                        for t in range(CAP + 1)
                    ]
                    band = bands[i, base + k]
                    lower = jnp.concatenate([band[:, :TILE], rest], axis=1)
                    term = jnp.dot(
                        jnp.concatenate(blocks, axis=0).astype(jnp.bfloat16),
                        jnp.concatenate([band, lower], axis=0),
                        preferred_element_type=jnp.float32,
                    )
                    total = term if total is None else total + term
                model_v[q] += total
            return carry

        lax.fori_loop(0, BAND // DOTS, group, 0)

    convolve(0, bands_even)
    convolve(1, bands_odd)

    load_seen.wait()
    for copy in copies[14:]:
        copy.wait_recv()

    down = lax.broadcasted_iota(jnp.int32, (BAND, TILE), 0) + r * BAND
    column = lax.broadcasted_iota(jnp.int32, (BAND, TILE), 1)
    parts = []
    for q in range(SPAN):
        start, length, first = runs[q]
        strips = []
        for t in range(CAP + 1):
            acc = model_v[q, pl.ds(t * BAND, BAND), :]
            part = acc[:, :TILE] + acc[:, TILE:]
            strips.append(pltpu.roll(part, TILE - (TILE - STEP) * t, 1) if t else part)
        for k in range(CAP):
            model = jnp.where(column < STEP - (TILE - STEP) * k, strips[k], strips[k + 1])
            pixels = seen[q, :, pl.ds(k * TILE, TILE)]
            if k == 0 and q > 0:
                pixels = jnp.where(start == q, pixels, seen[q, :, pl.ds(2 * TILE, TILE)])
            c = jnp.clip(start + k, 0, TILES - 1)
            residual = jnp.where(
                down < int_s[q, 0, 12 + c], pixels - model - float_s[q, 0, NB], 0.0
            )
            parts.append((jnp.where(k < length, first + k, -1), residual))
    for s in range(TILES):
        total = jnp.zeros((BAND, TILE), jnp.float32)
        tally = jnp.float32(0.0)
        for slot, residual in parts:
            total = total + jnp.where(slot == s, residual, 0.0)
            tally = tally + jnp.where(slot == s, 1.0, 0.0)
        out[0, s] = total
        tally_out[0, s] = jnp.full((BAND, TILE), jnp.maximum(tally, 1.0), jnp.float32)

    for copy in copies:
        copy.wait_send()


def solution(mesh):
    det_count, row_count = mesh.shape["det"], mesh.shape["row"]

    def body(
        science, template, sources, offsets, weights, valid, basis, coefs, background
    ):
        vmem = pl.BlockSpec(memory_space=pltpu.VMEM)
        hbm = pl.BlockSpec(memory_space=pltpu.HBM)
        total, tally = pl.pallas_call(
            functools.partial(kernel, det_count, row_count),
            out_shape=(
                jax.ShapeDtypeStruct(template.shape, jnp.float32),
                jax.ShapeDtypeStruct(template.shape, jnp.float32),
            ),
            in_specs=[hbm] * 8 + [pl.BlockSpec(memory_space=pltpu.SMEM)],
            out_specs=(vmem, vmem),
            scratch_shapes=[
                pltpu.VMEM((TILES, BAND, TILE), jnp.float32),
                pltpu.VMEM((ZERO_TILE + 1, DEEP, TILE), jnp.float32),
                pltpu.VMEM((2, BAND, TILE), jnp.float32),
                pltpu.VMEM((SPAN, 2, CAP + 1, 2 * BAND, TILE), jnp.float32),
                pltpu.VMEM((SPAN, BAND, CAP * TILE), jnp.float32),
                pltpu.VMEM((2, BAND, TILE, 2 * TILE), jnp.bfloat16),
                pltpu.VMEM((2, BAND, TILE, 2 * TILE), jnp.bfloat16),
                pltpu.VMEM((NB, KW, KW), jnp.float32),
                pltpu.VMEM((SPAN, (CAP + 1) * BAND, 2 * TILE), jnp.float32),
                pltpu.VMEM((BAND, TILE), jnp.float32),
                pltpu.VMEM((SPAN, BAND, TILE), jnp.float32),
                pltpu.VMEM((SPAN, 1, TILE), jnp.float32),
                pltpu.VMEM((SPAN, 1, TILE), jnp.int32),
                pltpu.SMEM((SPAN, 1, TILE), jnp.float32),
                pltpu.SMEM((SPAN, 1, TILE), jnp.int32),
                pltpu.SMEM((TILES, TILE), jnp.int32),
                pltpu.SMEM((2, 1, TILES), jnp.int32),
                pltpu.SMEM((2, 1, TILES), jnp.float32),
                pltpu.SMEM((1, TILES), jnp.int32),
                pltpu.SMEM((1, NB), jnp.float32),
                pltpu.SemaphoreType.DMA((11,)),
                pltpu.SemaphoreType.DMA((17,)),
                pltpu.SemaphoreType.DMA((17,)),
            ],
            compiler_params=pltpu.CompilerParams(
                collective_id=0, has_side_effects=True, vmem_limit_bytes=54 << 20
            ),
        )(
            science,
            template,
            sources.T,
            offsets,
            weights,
            valid,
            basis,
            coefs,
            background,
        )
        return total / tally

    in_specs = (
        P("det", "row", None),
        P("det", None, "row", None),
        P(),
        P(None, "det", None),
        P(None, "det", None),
        P("det", None),
        P(),
        P("det", None),
        P("det"),
    )
    out_specs = P("det", None, "row", None)
    return jax.shard_map(body, mesh=mesh, in_specs=in_specs, out_specs=out_specs, check_vma=False)
```

```python
import functools

import jax
import jax.numpy as jnp
from jax import lax
from jax.experimental import pallas as pl
from jax.experimental.pallas import tpu as pltpu
from jax.sharding import PartitionSpec as P

MESH = pl.DeviceIdType.MESH
SPAN = 4
CAP = 3
TILES = 6
TILE = 128
BAND = 32
ABOVE = 16
BELOW = 24
DEEP = ABOVE + BAND + BELOW
KW = 31
HALF = 15
NB = 27
AFTER = 19
GROUP = 8
DOTS = 32
MAXOFF = 4
STEP = 96
STRIP = 32
LEFT, RIGHT, ZERO_TILE = 6, 7, 8


def split(x):
    high = x.astype(jnp.bfloat16).astype(jnp.float32)
    return high, x - high


def kernel(
    det_count,
    row_count,
    science,
    template,
    sources,
    offsets,
    weights,
    valid,
    basis,
    coefs,
    background,
    out,
    own,
    tiles,
    edges,
    images,
    seen,
    bands_even,
    bands_odd,
    basis_v,
    model_v,
    taps,
    taps_back,
    floats,
    ints,
    float_s,
    int_s,
    sources_s,
    offsets_s,
    weights_s,
    valid_s,
    coefs_s,
    local_sem,
    send_sem,
    recv_sem,
):
    p = lax.axis_index("det")
    r = lax.axis_index("row")

    def det(j):
        return lax.rem(p + (j + det_count), det_count)

    def row(j):
        return lax.rem(r + (j + row_count), row_count)

    peers = [(det(j), r) for j in (1, -1, 2, -2, 3, -3)]
    peers += [(p, row(1)), (p, row(-1))]
    peers += [(det(j), row(i)) for j in (1, -1) for i in (1, -1)]
    barrier = pltpu.get_barrier_semaphore()
    for peer in peers:
        pl.semaphore_signal(barrier, inc=1, device_id=peer, device_id_type=MESH)

    load_own = pltpu.make_async_copy(template.at[0], own, local_sem.at[0])
    load_tiles = pltpu.make_async_copy(
        template.at[0], tiles.at[pl.ds(0, TILES), pl.ds(ABOVE, BAND), :], local_sem.at[1]
    )
    load_seen = pltpu.make_async_copy(
        science.at[0, :, pl.ds(0, CAP * TILE)], seen.at[0], local_sem.at[2]
    )
    load_basis = pltpu.make_async_copy(basis, basis_v, local_sem.at[5])
    small = []
    for i, (src, dst) in enumerate(
        (
            (sources, sources_s),
            (offsets, offsets_s),
            (weights, weights_s),
            (valid, valid_s),
            (coefs, coefs_s),
        )
    ):
        small.append(pltpu.make_async_copy(src, dst, local_sem.at[6 + i]))
    load_own.start()
    for copy in small:
        copy.start()
    load_basis.start()
    load_tiles.start()
    load_seen.start()
    for copy in small:
        copy.wait()

    lane = lax.broadcasted_iota(jnp.int32, (1, TILE), 1)
    packed = jnp.zeros((1, TILE), jnp.float32)
    whole = jnp.zeros((1, TILE), jnp.int32)
    for k in range(NB):
        packed = jnp.where(lane == k, coefs_s[0, k], packed)
    packed = jnp.where(lane == NB, background[0], packed)
    for c in range(TILES):
        packed = jnp.where(lane == 28 + c, weights_s[0, 0, c], packed)
        packed = jnp.where(lane == 34 + c, weights_s[1, 0, c], packed)
        whole = jnp.where(lane == c, offsets_s[0, 0, c], whole)
        whole = jnp.where(lane == 6 + c, offsets_s[1, 0, c], whole)
        whole = jnp.where(lane == 12 + c, valid_s[0, c], whole)
    floats[0] = packed
    ints[0] = whole

    load_own.wait()
    pl.semaphore_wait(barrier, len(peers))

    copies = []

    def always(action):
        action()

    def to_above(action):
        pl.when(r > 0)(action)

    def to_below(action):
        pl.when(r < row_count - 1)(action)

    def send(src, dst, peer, out=always, back=always):
        i = len(copies)
        copy = pltpu.make_async_remote_copy(
            src_ref=src,
            dst_ref=dst,
            send_sem=send_sem.at[i],
            recv_sem=recv_sem.at[i],
            device_id=peer,
            device_id_type=MESH,
        )
        out(lambda: copy.start())
        copies.append((copy, out, back))

    def arrived(group):
        for copy, out_of, back in group:
            back(lambda copy=copy: copy.wait_recv())

    low_rows, high_rows = pl.ds(ABOVE - HALF, HALF), pl.ds(ABOVE + BAND, AFTER)
    send(own.at[:, pl.ds(0, AFTER), :], tiles.at[pl.ds(0, TILES), high_rows, :],
        (p, row(-1)),
        to_above,
        to_below,
    )
    send(
        own.at[:, pl.ds(BAND - HALF, HALF), :],
        tiles.at[pl.ds(0, TILES), low_rows, :],
        (p, row(1)),
        to_below,
        to_above,
    )
    for j in range(1, SPAN):
        send(floats.at[0], floats.at[j], (det(j), r))
        send(ints.at[0], ints.at[j], (det(j), r))

    runs = []
    for q in range(SPAN):
        d = det(-q)
        start = jnp.int32(0)
        length = jnp.int32(0)
        for c in range(TILES):
            reach = lax.rem(sources_s[c, d] // TILES - d + det_count, det_count)
            start = start + jnp.where(reach < q, 1, 0)
            length = length + jnp.where(reach == q, 1, 0)
        start = jnp.clip(start, 0, TILES - 1)
        first = jnp.clip(sources_s[start, d] - p * TILES, 0, TILES - 1)
        runs.append((start, length, first))

    tiles[ZERO_TILE] = jnp.zeros((DEEP, TILE), jnp.float32)
    strip = lax.broadcasted_iota(jnp.int32, (BAND, TILE), 1) // STRIP
    ends = jnp.zeros((BAND, TILE), jnp.float32)
    begins = jnp.zeros((BAND, TILE), jnp.float32)
    for j in range(CAP):
        start, length, first = runs[j]
        last = own[jnp.clip(first + length - 1, 0, TILES - 1)]
        ends = jnp.where(strip == j, pltpu.roll(last, STRIP * (j + 1), 1), ends)
        start, length, first = runs[j + 1]
        head = own[first]
        begins = jnp.where(strip == j, pltpu.roll(head, STRIP * j, 1) if j else head, begins)
    edges[0] = ends
    edges[1] = begins

    for side, j, at in ((0, 1, LEFT), (1, -1, RIGHT)):
        send(
            edges.at[side, pl.ds(0, AFTER), :],
            tiles.at[at, high_rows, :],
            (det(j), row(-1)),
            to_above,
            to_below,
        )
        send(
            edges.at[side, pl.ds(BAND - HALF, HALF), :],
            tiles.at[at, low_rows, :],
            (det(j), row(1)),
            to_below,
            to_above,
        )
        send(edges.at[side], tiles.at[at, pl.ds(ABOVE, BAND), :], (det(j), r))
    for j in range(1, SPAN):
        send(
            science.at[0, :, pl.ds(j * TILE, CAP * TILE)],
            seen.at[j],
            (det(j), r),
        )


    def mirrored(first, last, coefficient):
        halves = []
        for q in range(first, last):
            total = coefficient(q, 0) * basis_v[0]
            for k in range(1, NB):
                total = total + coefficient(q, k) * basis_v[k]
            taps[q, pl.ds(0, KW), pl.ds(0, KW)] = total
        for q in range(first, last):
            halves += split(taps[q])
        both = jnp.dot(
            jnp.concatenate(halves, axis=0), mirror, preferred_element_type=jnp.float32
        )
        for q in range(first, last):
            at = 2 * BAND * (q - first)
            taps_back[q] = both[at : at + BAND] + both[at + BAND : at + 2 * BAND]

    def toeplitz(q, a, bands, place):
        line = jnp.broadcast_to(taps_back[q, pl.ds(a, 1), :], (8, TILE))
        block = pltpu.roll(line, 0, 1, stride=1, stride_axis=0)
        for jb in range(TILE // 16):
            turned = jnp.concatenate(
                [
                    block if shift == 0 else pltpu.roll(block, shift, 1)
                    for shift in (16 * jb, 16 * jb + 8)
                ],
                axis=0,
            )
            high = turned.astype(jnp.bfloat16)
            low = (turned - high.astype(jnp.float32)).astype(jnp.bfloat16)
            bands[place, a, pl.ds(16 * jb, 16), pl.ds(0, TILE)] = high
            bands[place, a, pl.ds(16 * jb, 16), pl.ds(TILE, TILE)] = low

    def toeplitz_first_pair(q):
        def group(step, carry):
            for k in range(GROUP):
                toeplitz(q, step * GROUP + k, bands_even, q)
            return carry

        lax.fori_loop(0, BAND // GROUP, group, 0)

    rows128 = lax.broadcasted_iota(jnp.int32, (TILE, TILE), 0)
    cols128 = lax.broadcasted_iota(jnp.int32, (TILE, TILE), 1)
    mirror = jnp.where(lax.rem(rows128 + cols128, TILE) == 0, 1.0, 0.0).astype(jnp.float32)
    taps[...] = jnp.zeros((SPAN, BAND, TILE), jnp.float32)
    load_basis.wait()
    mirrored(0, 1, lambda q, k: coefs_s[0, k])
    toeplitz_first_pair(0)
    arrived(copies[2:8])
    to_float = pltpu.make_async_copy(floats, float_s, local_sem.at[3])
    to_int = pltpu.make_async_copy(ints, int_s, local_sem.at[4])
    to_float.start()
    to_int.start()
    to_float.wait()
    to_int.wait()
    mirrored(1, SPAN, lambda q, k: float_s[q, 0, k])
    toeplitz_first_pair(1)
    load_tiles.wait()
    arrived(copies[:2] + copies[8:14])

    eight = lax.broadcasted_iota(jnp.int32, (2 * BAND, TILE), 0)
    wide = lax.broadcasted_iota(jnp.int32, (2 * BAND, TILE), 1)
    line_at = eight + (r * BAND - HALF)
    tail = wide < HALF
    for q in range(SPAN):
        start, length, first = runs[q]
        before = former = None
        for m in range(CAP + 2):
            c = jnp.clip(start + (m - 1), 0, TILES - 1)
            row_shift = jnp.clip(int_s[q, 0, c], 0, MAXOFF - 1)
            col_shift = int_s[q, 0, 6 + c]
            row_weight, col_weight = float_s[q, 0, 28 + c], float_s[q, 0, 34 + c]
            turn = jnp.int32(HALF + TILE) - col_shift
            last_lane = TILE - 1
            if m == 0:
                index = LEFT if q > 0 else ZERO_TILE
                last_lane = STRIP * q - 1 if q > 0 else TILE - 1
                turn = turn - STRIP * q
            else:
                edge = RIGHT if q < SPAN - 1 else ZERO_TILE
                index = jnp.where(
                    m <= length, first + (m - 1), jnp.where(m == length + 1, edge, ZERO_TILE)
                )
                index = jnp.clip(index, 0, ZERO_TILE)
                if q > 0:
                    turn = turn - jnp.where(m > length, STRIP * q, 0)
            upper = tiles[index, pl.ds(1 + row_shift, 2 * BAND), :]
            lower = tiles[index, pl.ds(2 + row_shift, 2 * BAND), :]
            limit = row_count * BAND - row_shift
            upper = jnp.where(line_at < limit, (1.0 - row_weight) * upper, 0.0)
            lower = jnp.where(line_at < limit - 1, row_weight * lower, 0.0)
            mixed = jnp.where(line_at >= 0, upper + lower, 0.0)
            last = jnp.broadcast_to(mixed[:, last_lane : last_lane + 1], (2 * BAND, TILE))
            left = pltpu.roll(mixed, lax.rem(turn, TILE), 1)
            left = jnp.where(tail & (wide > HALF - 1 - col_shift), last, left)
            following = pltpu.roll(mixed, lax.rem(turn - 1, TILE), 1)
            following = jnp.where(tail & (wide > HALF - 2 - col_shift), last, following)
            now = (1.0 - col_weight) * left + col_weight * following
            if m > 0:
                t = m - 1
                here = jnp.where(tail, before, now)
                window = here
                if t > 0:
                    skip = TILE - STEP
                    window = jnp.where(wide >= TILE - skip * t, former, here)
                    window = pltpu.roll(window, skip * t, 1)
                high, low = split(window)
                images[q, 0, t] = high
                images[q, 1, t] = low
                former = here
            before = now

    rest = jnp.zeros((TILE, TILE), jnp.bfloat16)
    model_v[...] = jnp.zeros_like(model_v)

    def convolve(pair, bands):
        def group(step, carry):
            base = step * DOTS
            for i in range(2):
                q = 2 * pair + i
                if pair == 0:
                    for k in range(DOTS):
                        toeplitz(q + 2, base + k, bands_odd, i)
                total = None
                for k in range(DOTS):
                    blocks = [
                        jnp.concatenate(
                            [images[q, part, t, pl.ds(base + k, BAND), :] for part in range(2)],
                            axis=1,
                        )
                        for t in range(CAP + 1)
                    ]
                    band = bands[i, base + k]
                    lower = jnp.concatenate([band[:, :TILE], rest], axis=1)
                    term = jnp.dot(
                        jnp.concatenate(blocks, axis=0).astype(jnp.bfloat16),
                        jnp.concatenate([band, lower], axis=0),
                        preferred_element_type=jnp.float32,
                    )
                    total = term if total is None else total + term
                model_v[q] += total
            return carry

        lax.fori_loop(0, BAND // DOTS, group, 0)

    convolve(0, bands_even)
    convolve(1, bands_odd)

    load_seen.wait()
    arrived(copies[14:])

    down = lax.broadcasted_iota(jnp.int32, (BAND, TILE), 0) + r * BAND
    column = lax.broadcasted_iota(jnp.int32, (BAND, TILE), 1)
    parts = []
    for q in range(SPAN):
        start, length, first = runs[q]
        strips = []
        for t in range(CAP + 1):
            acc = model_v[q, pl.ds(t * BAND, BAND), :]
            part = acc[:, :TILE] + acc[:, TILE:]
            strips.append(pltpu.roll(part, TILE - (TILE - STEP) * t, 1) if t else part)
        for k in range(CAP):
            model = jnp.where(column < STEP - (TILE - STEP) * k, strips[k], strips[k + 1])
            pixels = seen[q, :, pl.ds(k * TILE, TILE)]
            if k == 0 and q > 0:
                pixels = jnp.where(start == q, pixels, seen[q, :, pl.ds(2 * TILE, TILE)])
            c = jnp.clip(start + k, 0, TILES - 1)
            residual = jnp.where(
                down < int_s[q, 0, 12 + c], pixels - model - float_s[q, 0, NB], 0.0
            )
            parts.append((jnp.where(k < length, first + k, -1), residual))
    for s in range(TILES):
        total = jnp.zeros((BAND, TILE), jnp.float32)
        tally = jnp.float32(0.0)
        for slot, residual in parts:
            total = total + jnp.where(slot == s, residual, 0.0)
            tally = tally + jnp.where(slot == s, 1.0, 0.0)
        out[0, s] = total / jnp.maximum(tally, 1.0)

    for copy, out_of, back in copies:
        out_of(lambda copy=copy: copy.wait_send())


def solution(mesh):
    det_count, row_count = mesh.shape["det"], mesh.shape["row"]

    def body(
        science, template, sources, offsets, weights, valid, basis, coefs, background
    ):
        vmem = pl.BlockSpec(memory_space=pltpu.VMEM)
        hbm = pl.BlockSpec(memory_space=pltpu.HBM)
        return pl.pallas_call(
            functools.partial(kernel, det_count, row_count),
            out_shape=jax.ShapeDtypeStruct(template.shape, jnp.float32),
            in_specs=[hbm] * 8 + [pl.BlockSpec(memory_space=pltpu.SMEM)],
            out_specs=vmem,
            scratch_shapes=[
                pltpu.VMEM((TILES, BAND, TILE), jnp.float32),
                pltpu.VMEM((ZERO_TILE + 1, DEEP, TILE), jnp.float32),
                pltpu.VMEM((2, BAND, TILE), jnp.float32),
                pltpu.VMEM((SPAN, 2, CAP + 1, 2 * BAND, TILE), jnp.float32),
                pltpu.VMEM((SPAN, BAND, CAP * TILE), jnp.float32),
                pltpu.VMEM((2, BAND, TILE, 2 * TILE), jnp.bfloat16),
                pltpu.VMEM((2, BAND, TILE, 2 * TILE), jnp.bfloat16),
                pltpu.VMEM((NB, KW, KW), jnp.float32),
                pltpu.VMEM((SPAN, (CAP + 1) * BAND, 2 * TILE), jnp.float32),
                pltpu.VMEM((SPAN, BAND, TILE), jnp.float32),
                pltpu.VMEM((SPAN, BAND, TILE), jnp.float32),
                pltpu.VMEM((SPAN, 1, TILE), jnp.float32),
                pltpu.VMEM((SPAN, 1, TILE), jnp.int32),
                pltpu.SMEM((SPAN, 1, TILE), jnp.float32),
                pltpu.SMEM((SPAN, 1, TILE), jnp.int32),
                pltpu.SMEM((TILES, TILE), jnp.int32),
                pltpu.SMEM((2, 1, TILES), jnp.int32),
                pltpu.SMEM((2, 1, TILES), jnp.float32),
                pltpu.SMEM((1, TILES), jnp.int32),
                pltpu.SMEM((1, NB), jnp.float32),
                pltpu.SemaphoreType.DMA((11,)),
                pltpu.SemaphoreType.DMA((17,)),
                pltpu.SemaphoreType.DMA((17,)),
            ],
            compiler_params=pltpu.CompilerParams(
                collective_id=0, has_side_effects=True, vmem_limit_bytes=54 << 20
            ),
        )(
            science,
            template,
            sources.T,
            offsets,
            weights,
            valid,
            basis,
            coefs,
            background,
        )

    in_specs = (
        P("det", "row", None),
        P("det", None, "row", None),
        P(),
        P(None, "det", None),
        P(None, "det", None),
        P("det", None),
        P(),
        P("det", None),
        P("det"),
    )
    out_specs = P("det", None, "row", None)
    return jax.shard_map(body, mesh=mesh, in_specs=in_specs, out_specs=out_specs, check_vma=False)
```

```python
import functools

import jax
import jax.numpy as jnp
from jax import lax
from jax.experimental import pallas as pl
from jax.experimental.pallas import tpu as pltpu
from jax.sharding import PartitionSpec as P

MESH = pl.DeviceIdType.MESH
SPAN = 4
CAP = 3
TILES = 6
TILE = 128
BAND = 32
ABOVE = 16
BELOW = 24
DEEP = ABOVE + BAND + BELOW
KW = 31
HALF = 15
NB = 27
AFTER = 19
GROUP = 8
DOTS = 32
MAXOFF = 4
STEP = 96
STRIP = 32
LEFT, RIGHT, ZERO_TILE = 6, 7, 8


def split(x):
    high = x.astype(jnp.bfloat16).astype(jnp.float32)
    return high, x - high


def kernel(
    det_count,
    row_count,
    science,
    template,
    sources,
    offsets,
    weights,
    valid,
    basis,
    coefs,
    background,
    out,
    own,
    tiles,
    edges,
    images,
    seen,
    bands_even,
    bands_odd,
    basis_v,
    model_v,
    taps,
    taps_back,
    floats,
    ints,
    float_s,
    int_s,
    sources_s,
    offsets_s,
    weights_s,
    valid_s,
    coefs_s,
    local_sem,
    send_sem,
    recv_sem,
):
    p = lax.axis_index("det")
    r = lax.axis_index("row")

    def det(j):
        return lax.rem(p + (j + det_count), det_count)

    def row(j):
        return lax.rem(r + (j + row_count), row_count)

    peers = [(det(j), r) for j in (1, -1, 2, -2, 3, -3)]
    peers += [(p, row(1)), (p, row(-1))]
    peers += [(det(j), row(i)) for j in (1, -1) for i in (1, -1)]
    barrier = pltpu.get_barrier_semaphore()
    for peer in peers:
        pl.semaphore_signal(barrier, inc=1, device_id=peer, device_id_type=MESH)

    load_own = pltpu.make_async_copy(template.at[0], own, local_sem.at[0])
    load_tiles = pltpu.make_async_copy(
        template.at[0], tiles.at[pl.ds(0, TILES), pl.ds(ABOVE, BAND), :], local_sem.at[1]
    )
    load_seen = pltpu.make_async_copy(
        science.at[0, :, pl.ds(0, CAP * TILE)], seen.at[0], local_sem.at[2]
    )
    load_basis = pltpu.make_async_copy(basis, basis_v, local_sem.at[5])
    small = []
    for i, (src, dst) in enumerate(
        (
            (sources, sources_s),
            (offsets, offsets_s),
            (weights, weights_s),
            (valid, valid_s),
            (coefs, coefs_s),
        )
    ):
        small.append(pltpu.make_async_copy(src, dst, local_sem.at[6 + i]))
    for copy in small:
        copy.start()
    load_own.start()
    load_basis.start()
    load_tiles.start()
    load_seen.start()
    for copy in small:
        copy.wait()

    lane = lax.broadcasted_iota(jnp.int32, (1, TILE), 1)
    packed = jnp.zeros((1, TILE), jnp.float32)
    whole = jnp.zeros((1, TILE), jnp.int32)
    for k in range(NB):
        packed = jnp.where(lane == k, coefs_s[0, k], packed)
    packed = jnp.where(lane == NB, background[0], packed)
    for c in range(TILES):
        packed = jnp.where(lane == 28 + c, weights_s[0, 0, c], packed)
        packed = jnp.where(lane == 34 + c, weights_s[1, 0, c], packed)
        whole = jnp.where(lane == c, offsets_s[0, 0, c], whole)
        whole = jnp.where(lane == 6 + c, offsets_s[1, 0, c], whole)
        whole = jnp.where(lane == 12 + c, valid_s[0, c], whole)
    floats[0] = packed
    ints[0] = whole

    pl.semaphore_wait(barrier, len(peers))

    copies = []

    def always(action):
        action()

    def to_above(action):
        pl.when(r > 0)(action)

    def to_below(action):
        pl.when(r < row_count - 1)(action)

    def send(src, dst, peer, out=always, back=always):
        i = len(copies)
        copy = pltpu.make_async_remote_copy(
            src_ref=src,
            dst_ref=dst,
            send_sem=send_sem.at[i],
            recv_sem=recv_sem.at[i],
            device_id=peer,
            device_id_type=MESH,
        )
        out(lambda: copy.start())
        copies.append((copy, out, back))

    def arrived(group):
        for copy, out_of, back in group:
            back(lambda copy=copy: copy.wait_recv())

    for j in range(1, SPAN):
        send(floats.at[0], floats.at[j], (det(j), r))
        send(ints.at[0], ints.at[j], (det(j), r))
    load_own.wait()
    low_rows, high_rows = pl.ds(ABOVE - HALF, HALF), pl.ds(ABOVE + BAND, AFTER)
    send(own.at[:, pl.ds(0, AFTER), :], tiles.at[pl.ds(0, TILES), high_rows, :],
        (p, row(-1)),
        to_above,
        to_below,
    )
    send(
        own.at[:, pl.ds(BAND - HALF, HALF), :],
        tiles.at[pl.ds(0, TILES), low_rows, :],
        (p, row(1)),
        to_below,
        to_above,
    )

    runs = []
    for q in range(SPAN):
        d = det(-q)
        start = jnp.int32(0)
        length = jnp.int32(0)
        for c in range(TILES):
            reach = lax.rem(sources_s[c, d] // TILES - d + det_count, det_count)
            start = start + jnp.where(reach < q, 1, 0)
            length = length + jnp.where(reach == q, 1, 0)
        start = jnp.clip(start, 0, TILES - 1)
        first = jnp.clip(sources_s[start, d] - p * TILES, 0, TILES - 1)
        runs.append((start, length, first))

    tiles[ZERO_TILE] = jnp.zeros((DEEP, TILE), jnp.float32)
    strip = lax.broadcasted_iota(jnp.int32, (BAND, TILE), 1) // STRIP
    ends = jnp.zeros((BAND, TILE), jnp.float32)
    begins = jnp.zeros((BAND, TILE), jnp.float32)
    for j in range(CAP):
        start, length, first = runs[j]
        last = own[jnp.clip(first + length - 1, 0, TILES - 1)]
        ends = jnp.where(strip == j, pltpu.roll(last, STRIP * (j + 1), 1), ends)
        start, length, first = runs[j + 1]
        head = own[first]
        begins = jnp.where(strip == j, pltpu.roll(head, STRIP * j, 1) if j else head, begins)
    edges[0] = ends
    edges[1] = begins

    for side, j, at in ((0, 1, LEFT), (1, -1, RIGHT)):
        send(
            edges.at[side, pl.ds(0, AFTER), :],
            tiles.at[at, high_rows, :],
            (det(j), row(-1)),
            to_above,
            to_below,
        )
        send(
            edges.at[side, pl.ds(BAND - HALF, HALF), :],
            tiles.at[at, low_rows, :],
            (det(j), row(1)),
            to_below,
            to_above,
        )
        send(edges.at[side], tiles.at[at, pl.ds(ABOVE, BAND), :], (det(j), r))
    for j in range(1, SPAN):
        send(
            science.at[0, :, pl.ds(j * TILE, CAP * TILE)],
            seen.at[j],
            (det(j), r),
        )


    def mirrored(first, last, coefficient):
        halves = []
        for q in range(first, last):
            total = coefficient(q, 0) * basis_v[0]
            for k in range(1, NB):
                total = total + coefficient(q, k) * basis_v[k]
            taps[q, pl.ds(0, KW), pl.ds(0, KW)] = total
        for q in range(first, last):
            halves += split(taps[q])
        both = jnp.dot(
            jnp.concatenate(halves, axis=0), mirror, preferred_element_type=jnp.float32
        )
        for q in range(first, last):
            at = 2 * BAND * (q - first)
            taps_back[q] = both[at : at + BAND] + both[at + BAND : at + 2 * BAND]

    def toeplitz(q, a, bands, place):
        line = jnp.broadcast_to(taps_back[q, pl.ds(a, 1), :], (8, TILE))
        block = pltpu.roll(line, 0, 1, stride=1, stride_axis=0)
        for jb in range(TILE // 16):
            turned = jnp.concatenate(
                [
                    block if shift == 0 else pltpu.roll(block, shift, 1)
                    for shift in (16 * jb, 16 * jb + 8)
                ],
                axis=0,
            )
            high = turned.astype(jnp.bfloat16)
            low = (turned - high.astype(jnp.float32)).astype(jnp.bfloat16)
            bands[place, a, pl.ds(16 * jb, 16), pl.ds(0, TILE)] = high
            bands[place, a, pl.ds(16 * jb, 16), pl.ds(TILE, TILE)] = low

    def toeplitz_first_pair(q):
        def group(step, carry):
            for k in range(GROUP):
                toeplitz(q, step * GROUP + k, bands_even, q)
            return carry

        lax.fori_loop(0, BAND // GROUP, group, 0)

    rows128 = lax.broadcasted_iota(jnp.int32, (TILE, TILE), 0)
    cols128 = lax.broadcasted_iota(jnp.int32, (TILE, TILE), 1)
    mirror = jnp.where(lax.rem(rows128 + cols128, TILE) == 0, 1.0, 0.0).astype(jnp.float32)
    taps[...] = jnp.zeros((SPAN, BAND, TILE), jnp.float32)
    load_basis.wait()
    mirrored(0, 1, lambda q, k: coefs_s[0, k])
    toeplitz_first_pair(0)
    arrived(copies[:6])
    to_float = pltpu.make_async_copy(floats, float_s, local_sem.at[3])
    to_int = pltpu.make_async_copy(ints, int_s, local_sem.at[4])
    to_float.start()
    to_int.start()
    to_float.wait()
    to_int.wait()
    mirrored(1, SPAN, lambda q, k: float_s[q, 0, k])
    toeplitz_first_pair(1)
    load_tiles.wait()
    arrived(copies[6:14])

    eight = lax.broadcasted_iota(jnp.int32, (2 * BAND, TILE), 0)
    wide = lax.broadcasted_iota(jnp.int32, (2 * BAND, TILE), 1)
    line_at = eight + (r * BAND - HALF)
    tail = wide < HALF
    for q in range(SPAN):
        start, length, first = runs[q]
        before = former = None
        for m in range(CAP + 2):
            c = jnp.clip(start + (m - 1), 0, TILES - 1)
            row_shift = jnp.clip(int_s[q, 0, c], 0, MAXOFF - 1)
            col_shift = int_s[q, 0, 6 + c]
            row_weight, col_weight = float_s[q, 0, 28 + c], float_s[q, 0, 34 + c]
            turn = jnp.int32(HALF + TILE) - col_shift
            last_lane = TILE - 1
            if m == 0:
                index = LEFT if q > 0 else ZERO_TILE
                last_lane = STRIP * q - 1 if q > 0 else TILE - 1
                turn = turn - STRIP * q
            else:
                edge = RIGHT if q < SPAN - 1 else ZERO_TILE
                index = jnp.where(
                    m <= length, first + (m - 1), jnp.where(m == length + 1, edge, ZERO_TILE)
                )
                index = jnp.clip(index, 0, ZERO_TILE)
                if q > 0:
                    turn = turn - jnp.where(m > length, STRIP * q, 0)
            upper = tiles[index, pl.ds(1 + row_shift, 2 * BAND), :]
            lower = tiles[index, pl.ds(2 + row_shift, 2 * BAND), :]
            limit = row_count * BAND - row_shift
            upper = jnp.where(line_at < limit, (1.0 - row_weight) * upper, 0.0)
            lower = jnp.where(line_at < limit - 1, row_weight * lower, 0.0)
            mixed = jnp.where(line_at >= 0, upper + lower, 0.0)
            last = jnp.broadcast_to(mixed[:, last_lane : last_lane + 1], (2 * BAND, TILE))
            left = pltpu.roll(mixed, lax.rem(turn, TILE), 1)
            left = jnp.where(tail & (wide > HALF - 1 - col_shift), last, left)
            following = pltpu.roll(mixed, lax.rem(turn - 1, TILE), 1)
            following = jnp.where(tail & (wide > HALF - 2 - col_shift), last, following)
            now = (1.0 - col_weight) * left + col_weight * following
            if m > 0:
                t = m - 1
                here = jnp.where(tail, before, now)
                window = here
                if t > 0:
                    skip = TILE - STEP
                    window = jnp.where(wide >= TILE - skip * t, former, here)
                    window = pltpu.roll(window, skip * t, 1)
                high, low = split(window)
                images[q, 0, t] = high
                images[q, 1, t] = low
                former = here
            before = now

    rest = jnp.zeros((TILE, TILE), jnp.bfloat16)
    model_v[...] = jnp.zeros_like(model_v)

    def convolve(pair, bands):
        def group(step, carry):
            base = step * DOTS
            for i in range(2):
                q = 2 * pair + i
                if pair == 0:
                    for k in range(DOTS):
                        toeplitz(q + 2, base + k, bands_odd, i)
                total = None
                for k in range(DOTS):
                    blocks = [
                        jnp.concatenate(
                            [images[q, part, t, pl.ds(base + k, BAND), :] for part in range(2)],
                            axis=1,
                        )
                        for t in range(CAP + 1)
                    ]
                    band = bands[i, base + k]
                    lower = jnp.concatenate([band[:, :TILE], rest], axis=1)
                    term = jnp.dot(
                        jnp.concatenate(blocks, axis=0).astype(jnp.bfloat16),
                        jnp.concatenate([band, lower], axis=0),
                        preferred_element_type=jnp.float32,
                    )
                    total = term if total is None else total + term
                model_v[q] += total
            return carry

        lax.fori_loop(0, BAND // DOTS, group, 0)

    convolve(0, bands_even)
    convolve(1, bands_odd)

    load_seen.wait()
    arrived(copies[14:])

    down = lax.broadcasted_iota(jnp.int32, (BAND, TILE), 0) + r * BAND
    column = lax.broadcasted_iota(jnp.int32, (BAND, TILE), 1)
    parts = []
    for q in range(SPAN):
        start, length, first = runs[q]
        strips = []
        for t in range(CAP + 1):
            acc = model_v[q, pl.ds(t * BAND, BAND), :]
            part = acc[:, :TILE] + acc[:, TILE:]
            strips.append(pltpu.roll(part, TILE - (TILE - STEP) * t, 1) if t else part)
        for k in range(CAP):
            model = jnp.where(column < STEP - (TILE - STEP) * k, strips[k], strips[k + 1])
            pixels = seen[q, :, pl.ds(k * TILE, TILE)]
            if k == 0 and q > 0:
                pixels = jnp.where(start == q, pixels, seen[q, :, pl.ds(2 * TILE, TILE)])
            c = jnp.clip(start + k, 0, TILES - 1)
            residual = jnp.where(
                down < int_s[q, 0, 12 + c], pixels - model - float_s[q, 0, NB], 0.0
            )
            parts.append((jnp.where(k < length, first + k, -1), residual))
    for s in range(TILES):
        total = jnp.zeros((BAND, TILE), jnp.float32)
        tally = jnp.float32(0.0)
        for slot, residual in parts:
            total = total + jnp.where(slot == s, residual, 0.0)
            tally = tally + jnp.where(slot == s, 1.0, 0.0)
        out[0, s] = total / jnp.maximum(tally, 1.0)

    for copy, out_of, back in copies:
        out_of(lambda copy=copy: copy.wait_send())


def solution(mesh):
    det_count, row_count = mesh.shape["det"], mesh.shape["row"]

    def body(
        science, template, sources, offsets, weights, valid, basis, coefs, background
    ):
        vmem = pl.BlockSpec(memory_space=pltpu.VMEM)
        hbm = pl.BlockSpec(memory_space=pltpu.HBM)
        return pl.pallas_call(
            functools.partial(kernel, det_count, row_count),
            out_shape=jax.ShapeDtypeStruct(template.shape, jnp.float32),
            in_specs=[hbm] * 8 + [pl.BlockSpec(memory_space=pltpu.SMEM)],
            out_specs=vmem,
            scratch_shapes=[
                pltpu.VMEM((TILES, BAND, TILE), jnp.float32),
                pltpu.VMEM((ZERO_TILE + 1, DEEP, TILE), jnp.float32),
                pltpu.VMEM((2, BAND, TILE), jnp.float32),
                pltpu.VMEM((SPAN, 2, CAP + 1, 2 * BAND, TILE), jnp.float32),
                pltpu.VMEM((SPAN, BAND, CAP * TILE), jnp.float32),
                pltpu.VMEM((2, BAND, TILE, 2 * TILE), jnp.bfloat16),
                pltpu.VMEM((2, BAND, TILE, 2 * TILE), jnp.bfloat16),
                pltpu.VMEM((NB, KW, KW), jnp.float32),
                pltpu.VMEM((SPAN, (CAP + 1) * BAND, 2 * TILE), jnp.float32),
                pltpu.VMEM((SPAN, BAND, TILE), jnp.float32),
                pltpu.VMEM((SPAN, BAND, TILE), jnp.float32),
                pltpu.VMEM((SPAN, 1, TILE), jnp.float32),
                pltpu.VMEM((SPAN, 1, TILE), jnp.int32),
                pltpu.SMEM((SPAN, 1, TILE), jnp.float32),
                pltpu.SMEM((SPAN, 1, TILE), jnp.int32),
                pltpu.SMEM((TILES, TILE), jnp.int32),
                pltpu.SMEM((2, 1, TILES), jnp.int32),
                pltpu.SMEM((2, 1, TILES), jnp.float32),
                pltpu.SMEM((1, TILES), jnp.int32),
                pltpu.SMEM((1, NB), jnp.float32),
                pltpu.SemaphoreType.DMA((11,)),
                pltpu.SemaphoreType.DMA((17,)),
                pltpu.SemaphoreType.DMA((17,)),
            ],
            compiler_params=pltpu.CompilerParams(
                collective_id=0, has_side_effects=True, vmem_limit_bytes=54 << 20
            ),
        )(
            science,
            template,
            sources.T,
            offsets,
            weights,
            valid,
            basis,
            coefs,
            background,
        )

    in_specs = (
        P("det", "row", None),
        P("det", None, "row", None),
        P(),
        P(None, "det", None),
        P(None, "det", None),
        P("det", None),
        P(),
        P("det", None),
        P("det"),
    )
    out_specs = P("det", None, "row", None)
    return jax.shard_map(body, mesh=mesh, in_specs=in_specs, out_specs=out_specs, check_vma=False)
```

```python
import functools

import jax
import jax.numpy as jnp
from jax import lax
from jax.experimental import pallas as pl
from jax.experimental.pallas import tpu as pltpu
from jax.sharding import PartitionSpec as P

MESH = pl.DeviceIdType.MESH
SPAN = 4
CAP = 3
TILES = 6
TILE = 128
BAND = 32
ABOVE = 16
BELOW = 24
DEEP = ABOVE + BAND + BELOW
KW = 31
HALF = 15
NB = 27
AFTER = 19
GROUP = 8
DOTS = 32
MAXOFF = 4
STEP = 96
STRIP = 32
LEFT, RIGHT, ZERO_TILE = 6, 7, 8


def split(x):
    high = x.astype(jnp.bfloat16).astype(jnp.float32)
    return high, x - high


def kernel(
    det_count,
    row_count,
    science,
    template,
    sources,
    offsets,
    weights,
    valid,
    basis,
    coefs,
    background,
    out,
    own,
    tiles,
    edges,
    images,
    seen,
    bands_even,
    bands_odd,
    basis_v,
    model_v,
    taps,
    taps_back,
    floats,
    ints,
    float_s,
    int_s,
    sources_s,
    offsets_s,
    weights_s,
    valid_s,
    coefs_s,
    local_sem,
    send_sem,
    recv_sem,
):
    p = lax.axis_index("det")
    r = lax.axis_index("row")

    def det(j):
        return lax.rem(p + (j + det_count), det_count)

    def row(j):
        return lax.rem(r + (j + row_count), row_count)

    peers = [(det(j), r) for j in (1, -1, 2, -2, 3, -3)]
    peers += [(p, row(1)), (p, row(-1))]
    peers += [(det(j), row(i)) for j in (1, -1) for i in (1, -1)]
    barrier = pltpu.get_barrier_semaphore()
    for peer in peers:
        pl.semaphore_signal(barrier, inc=1, device_id=peer, device_id_type=MESH)

    load_own = pltpu.make_async_copy(template.at[0], own, local_sem.at[0])
    load_tiles = pltpu.make_async_copy(
        template.at[0], tiles.at[pl.ds(0, TILES), pl.ds(ABOVE, BAND), :], local_sem.at[1]
    )
    load_seen = pltpu.make_async_copy(
        science.at[0, :, pl.ds(0, CAP * TILE)], seen.at[0], local_sem.at[2]
    )
    load_basis = pltpu.make_async_copy(basis, basis_v, local_sem.at[5])
    small = []
    for i, (src, dst) in enumerate(
        (
            (sources, sources_s),
            (offsets, offsets_s),
            (weights, weights_s),
            (valid, valid_s),
            (coefs, coefs_s),
        )
    ):
        small.append(pltpu.make_async_copy(src, dst, local_sem.at[6 + i]))
    for copy in small:
        copy.start()
    load_own.start()
    load_basis.start()
    load_tiles.start()
    load_seen.start()
    for copy in small:
        copy.wait()

    lane = lax.broadcasted_iota(jnp.int32, (1, TILE), 1)
    packed = jnp.zeros((1, TILE), jnp.float32)
    whole = jnp.zeros((1, TILE), jnp.int32)
    for k in range(NB):
        packed = jnp.where(lane == k, coefs_s[0, k], packed)
    packed = jnp.where(lane == NB, background[0], packed)
    for c in range(TILES):
        packed = jnp.where(lane == 28 + c, weights_s[0, 0, c], packed)
        packed = jnp.where(lane == 34 + c, weights_s[1, 0, c], packed)
        whole = jnp.where(lane == c, offsets_s[0, 0, c], whole)
        whole = jnp.where(lane == 6 + c, offsets_s[1, 0, c], whole)
        whole = jnp.where(lane == 12 + c, valid_s[0, c], whole)
    floats[0] = packed
    ints[0] = whole

    pl.semaphore_wait(barrier, len(peers))

    copies = []

    def always(action):
        action()

    def to_above(action):
        pl.when(r > 0)(action)

    def to_below(action):
        pl.when(r < row_count - 1)(action)

    def send(src, dst, peer, out=always, back=always):
        i = len(copies)
        copy = pltpu.make_async_remote_copy(
            src_ref=src,
            dst_ref=dst,
            send_sem=send_sem.at[i],
            recv_sem=recv_sem.at[i],
            device_id=peer,
            device_id_type=MESH,
        )
        out(lambda: copy.start())
        copies.append((copy, out, back))

    def arrived(group):
        for copy, out_of, back in group:
            back(lambda copy=copy: copy.wait_recv())

    for j in range(1, SPAN):
        send(floats.at[0], floats.at[j], (det(j), r))
        send(ints.at[0], ints.at[j], (det(j), r))
    load_own.wait()
    low_rows, high_rows = pl.ds(ABOVE - HALF, HALF), pl.ds(ABOVE + BAND, AFTER)
    send(own.at[:, pl.ds(0, AFTER), :], tiles.at[pl.ds(0, TILES), high_rows, :],
        (p, row(-1)),
        to_above,
        to_below,
    )
    send(
        own.at[:, pl.ds(BAND - HALF, HALF), :],
        tiles.at[pl.ds(0, TILES), low_rows, :],
        (p, row(1)),
        to_below,
        to_above,
    )

    runs = []
    for q in range(SPAN):
        d = det(-q)
        start = jnp.int32(0)
        length = jnp.int32(0)
        for c in range(TILES):
            reach = lax.rem(sources_s[c, d] // TILES - d + det_count, det_count)
            start = start + jnp.where(reach < q, 1, 0)
            length = length + jnp.where(reach == q, 1, 0)
        start = jnp.clip(start, 0, TILES - 1)
        first = jnp.clip(sources_s[start, d] - p * TILES, 0, TILES - 1)
        runs.append((start, length, first))

    tiles[ZERO_TILE] = jnp.zeros((DEEP, TILE), jnp.float32)
    strip = lax.broadcasted_iota(jnp.int32, (BAND, TILE), 1) // STRIP
    ends = jnp.zeros((BAND, TILE), jnp.float32)
    begins = jnp.zeros((BAND, TILE), jnp.float32)
    for j in range(CAP):
        start, length, first = runs[j]
        last = own[jnp.clip(first + length - 1, 0, TILES - 1)]
        ends = jnp.where(strip == j, pltpu.roll(last, STRIP * (j + 1), 1), ends)
        start, length, first = runs[j + 1]
        head = own[first]
        begins = jnp.where(strip == j, pltpu.roll(head, STRIP * j, 1) if j else head, begins)
    edges[0] = ends
    edges[1] = begins

    for side, j, at in ((0, 1, LEFT), (1, -1, RIGHT)):
        send(
            edges.at[side, pl.ds(0, AFTER), :],
            tiles.at[at, high_rows, :],
            (det(j), row(-1)),
            to_above,
            to_below,
        )
        send(
            edges.at[side, pl.ds(BAND - HALF, HALF), :],
            tiles.at[at, low_rows, :],
            (det(j), row(1)),
            to_below,
            to_above,
        )
        send(edges.at[side], tiles.at[at, pl.ds(ABOVE, BAND), :], (det(j), r))
    for j in range(1, SPAN):
        send(
            science.at[0, :, pl.ds(j * TILE, CAP * TILE)],
            seen.at[j],
            (det(j), r),
        )


    def mirrored(first, last, coefficient):
        halves = []
        for q in range(first, last):
            total = coefficient(q, 0) * basis_v[0]
            for k in range(1, NB):
                total = total + coefficient(q, k) * basis_v[k]
            taps[q, pl.ds(0, KW), pl.ds(0, KW)] = total
        for q in range(first, last):
            halves += split(taps[q])
        both = jnp.dot(
            jnp.concatenate(halves, axis=0), mirror, preferred_element_type=jnp.float32
        )
        for q in range(first, last):
            at = 2 * BAND * (q - first)
            taps_back[q] = both[at : at + BAND] + both[at + BAND : at + 2 * BAND]

    def toeplitz(q, a, bands, place):
        line = jnp.broadcast_to(taps_back[q, pl.ds(a, 1), :], (8, TILE))
        block = pltpu.roll(line, 0, 1, stride=1, stride_axis=0)
        for jb in range(TILE // 16):
            turned = jnp.concatenate(
                [
                    block if shift == 0 else pltpu.roll(block, shift, 1)
                    for shift in (16 * jb, 16 * jb + 8)
                ],
                axis=0,
            )
            high = turned.astype(jnp.bfloat16)
            low = (turned - high.astype(jnp.float32)).astype(jnp.bfloat16)
            bands[place, a, pl.ds(16 * jb, 16), pl.ds(0, TILE)] = high
            bands[place, a, pl.ds(16 * jb, 16), pl.ds(TILE, TILE)] = low

    def toeplitz_first_pair(q):
        def group(step, carry):
            for k in range(GROUP):
                toeplitz(q, step * GROUP + k, bands_even, q)
            return carry

        lax.fori_loop(0, BAND // GROUP, group, 0)

    rows128 = lax.broadcasted_iota(jnp.int32, (TILE, TILE), 0)
    cols128 = lax.broadcasted_iota(jnp.int32, (TILE, TILE), 1)
    mirror = jnp.where(lax.rem(rows128 + cols128, TILE) == 0, 1.0, 0.0).astype(jnp.float32)
    taps[...] = jnp.zeros((SPAN, BAND, TILE), jnp.float32)
    load_basis.wait()
    mirrored(0, 1, lambda q, k: coefs_s[0, k])
    toeplitz_first_pair(0)
    load_tiles.wait()
    arrived(copies[6:14])
    eight = lax.broadcasted_iota(jnp.int32, (2 * BAND, TILE), 0)
    wide = lax.broadcasted_iota(jnp.int32, (2 * BAND, TILE), 1)
    line_at = eight + (r * BAND - HALF)
    tail = wide < HALF
    def own_shift(c):
        return (
            (offsets_s[0, 0, c], offsets_s[1, 0, c]),
            (weights_s[0, 0, c], weights_s[1, 0, c]),
        )

    def sent_shift(q, c):
        return (
            (int_s[q, 0, c], int_s[q, 0, 6 + c]),
            (float_s[q, 0, 28 + c], float_s[q, 0, 34 + c]),
        )

    def warp(kernels):
        for q in kernels:
            start, length, first = runs[q]
            before = former = None
            for m in range(CAP + 2):
                c = jnp.clip(start + (m - 1), 0, TILES - 1)
                shifts, mixes = own_shift(c) if q == 0 else sent_shift(q, c)
                row_shift = jnp.clip(shifts[0], 0, MAXOFF - 1)
                col_shift = shifts[1]
                row_weight, col_weight = mixes
                turn = jnp.int32(HALF + TILE) - col_shift
                last_lane = TILE - 1
                if m == 0:
                    index = LEFT if q > 0 else ZERO_TILE
                    last_lane = STRIP * q - 1 if q > 0 else TILE - 1
                    turn = turn - STRIP * q
                else:
                    edge = RIGHT if q < SPAN - 1 else ZERO_TILE
                    index = jnp.where(
                        m <= length, first + (m - 1), jnp.where(m == length + 1, edge, ZERO_TILE)
                    )
                    index = jnp.clip(index, 0, ZERO_TILE)
                    if q > 0:
                        turn = turn - jnp.where(m > length, STRIP * q, 0)
                upper = tiles[index, pl.ds(1 + row_shift, 2 * BAND), :]
                lower = tiles[index, pl.ds(2 + row_shift, 2 * BAND), :]
                limit = row_count * BAND - row_shift
                upper = jnp.where(line_at < limit, (1.0 - row_weight) * upper, 0.0)
                lower = jnp.where(line_at < limit - 1, row_weight * lower, 0.0)
                mixed = jnp.where(line_at >= 0, upper + lower, 0.0)
                last = jnp.broadcast_to(mixed[:, last_lane : last_lane + 1], (2 * BAND, TILE))
                left = pltpu.roll(mixed, lax.rem(turn, TILE), 1)
                left = jnp.where(tail & (wide > HALF - 1 - col_shift), last, left)
                following = pltpu.roll(mixed, lax.rem(turn - 1, TILE), 1)
                following = jnp.where(tail & (wide > HALF - 2 - col_shift), last, following)
                now = (1.0 - col_weight) * left + col_weight * following
                if m > 0:
                    t = m - 1
                    here = jnp.where(tail, before, now)
                    window = here
                    if t > 0:
                        skip = TILE - STEP
                        window = jnp.where(wide >= TILE - skip * t, former, here)
                        window = pltpu.roll(window, skip * t, 1)
                    high, low = split(window)
                    images[q, 0, t] = high
                    images[q, 1, t] = low
                    former = here
                before = now

    warp(range(1))
    arrived(copies[:6])
    to_float = pltpu.make_async_copy(floats, float_s, local_sem.at[3])
    to_int = pltpu.make_async_copy(ints, int_s, local_sem.at[4])
    to_float.start()
    to_int.start()
    to_float.wait()
    to_int.wait()
    mirrored(1, SPAN, lambda q, k: float_s[q, 0, k])
    toeplitz_first_pair(1)

    warp(range(1, SPAN))

    rest = jnp.zeros((TILE, TILE), jnp.bfloat16)
    model_v[...] = jnp.zeros_like(model_v)

    def convolve(pair, bands):
        def group(step, carry):
            base = step * DOTS
            for i in range(2):
                q = 2 * pair + i
                if pair == 0:
                    for k in range(DOTS):
                        toeplitz(q + 2, base + k, bands_odd, i)
                total = None
                for k in range(DOTS):
                    blocks = [
                        jnp.concatenate(
                            [images[q, part, t, pl.ds(base + k, BAND), :] for part in range(2)],
                            axis=1,
                        )
                        for t in range(CAP + 1)
                    ]
                    band = bands[i, base + k]
                    lower = jnp.concatenate([band[:, :TILE], rest], axis=1)
                    term = jnp.dot(
                        jnp.concatenate(blocks, axis=0).astype(jnp.bfloat16),
                        jnp.concatenate([band, lower], axis=0),
                        preferred_element_type=jnp.float32,
                    )
                    total = term if total is None else total + term
                model_v[q] += total
            return carry

        lax.fori_loop(0, BAND // DOTS, group, 0)

    convolve(0, bands_even)
    convolve(1, bands_odd)

    load_seen.wait()
    arrived(copies[14:])

    down = lax.broadcasted_iota(jnp.int32, (BAND, TILE), 0) + r * BAND
    column = lax.broadcasted_iota(jnp.int32, (BAND, TILE), 1)
    parts = []
    for q in range(SPAN):
        start, length, first = runs[q]
        strips = []
        for t in range(CAP + 1):
            acc = model_v[q, pl.ds(t * BAND, BAND), :]
            part = acc[:, :TILE] + acc[:, TILE:]
            strips.append(pltpu.roll(part, TILE - (TILE - STEP) * t, 1) if t else part)
        for k in range(CAP):
            model = jnp.where(column < STEP - (TILE - STEP) * k, strips[k], strips[k + 1])
            pixels = seen[q, :, pl.ds(k * TILE, TILE)]
            if k == 0 and q > 0:
                pixels = jnp.where(start == q, pixels, seen[q, :, pl.ds(2 * TILE, TILE)])
            c = jnp.clip(start + k, 0, TILES - 1)
            residual = jnp.where(
                down < int_s[q, 0, 12 + c], pixels - model - float_s[q, 0, NB], 0.0
            )
            parts.append((jnp.where(k < length, first + k, -1), residual))
    for s in range(TILES):
        total = jnp.zeros((BAND, TILE), jnp.float32)
        tally = jnp.float32(0.0)
        for slot, residual in parts:
            total = total + jnp.where(slot == s, residual, 0.0)
            tally = tally + jnp.where(slot == s, 1.0, 0.0)
        out[0, s] = total / jnp.maximum(tally, 1.0)

    for copy, out_of, back in copies:
        out_of(lambda copy=copy: copy.wait_send())


def solution(mesh):
    det_count, row_count = mesh.shape["det"], mesh.shape["row"]

    def body(
        science, template, sources, offsets, weights, valid, basis, coefs, background
    ):
        vmem = pl.BlockSpec(memory_space=pltpu.VMEM)
        hbm = pl.BlockSpec(memory_space=pltpu.HBM)
        return pl.pallas_call(
            functools.partial(kernel, det_count, row_count),
            out_shape=jax.ShapeDtypeStruct(template.shape, jnp.float32),
            in_specs=[hbm] * 8 + [pl.BlockSpec(memory_space=pltpu.SMEM)],
            out_specs=vmem,
            scratch_shapes=[
                pltpu.VMEM((TILES, BAND, TILE), jnp.float32),
                pltpu.VMEM((ZERO_TILE + 1, DEEP, TILE), jnp.float32),
                pltpu.VMEM((2, BAND, TILE), jnp.float32),
                pltpu.VMEM((SPAN, 2, CAP + 1, 2 * BAND, TILE), jnp.float32),
                pltpu.VMEM((SPAN, BAND, CAP * TILE), jnp.float32),
                pltpu.VMEM((2, BAND, TILE, 2 * TILE), jnp.bfloat16),
                pltpu.VMEM((2, BAND, TILE, 2 * TILE), jnp.bfloat16),
                pltpu.VMEM((NB, KW, KW), jnp.float32),
                pltpu.VMEM((SPAN, (CAP + 1) * BAND, 2 * TILE), jnp.float32),
                pltpu.VMEM((SPAN, BAND, TILE), jnp.float32),
                pltpu.VMEM((SPAN, BAND, TILE), jnp.float32),
                pltpu.VMEM((SPAN, 1, TILE), jnp.float32),
                pltpu.VMEM((SPAN, 1, TILE), jnp.int32),
                pltpu.SMEM((SPAN, 1, TILE), jnp.float32),
                pltpu.SMEM((SPAN, 1, TILE), jnp.int32),
                pltpu.SMEM((TILES, TILE), jnp.int32),
                pltpu.SMEM((2, 1, TILES), jnp.int32),
                pltpu.SMEM((2, 1, TILES), jnp.float32),
                pltpu.SMEM((1, TILES), jnp.int32),
                pltpu.SMEM((1, NB), jnp.float32),
                pltpu.SemaphoreType.DMA((11,)),
                pltpu.SemaphoreType.DMA((17,)),
                pltpu.SemaphoreType.DMA((17,)),
            ],
            compiler_params=pltpu.CompilerParams(
                collective_id=0, has_side_effects=True, vmem_limit_bytes=54 << 20
            ),
        )(
            science,
            template,
            sources.T,
            offsets,
            weights,
            valid,
            basis,
            coefs,
            background,
        )

    in_specs = (
        P("det", "row", None),
        P("det", None, "row", None),
        P(),
        P(None, "det", None),
        P(None, "det", None),
        P("det", None),
        P(),
        P("det", None),
        P("det"),
    )
    out_specs = P("det", None, "row", None)
    return jax.shard_map(body, mesh=mesh, in_specs=in_specs, out_specs=out_specs, check_vma=False)
```
